256 devices in a mesh: mem: 32 (over x_lo, z, core), space: 8 (over x_hi, y).
Axes of the slice: x: 4 (x_hi: 2, x_lo: 2; x = x_hi * 2 + x_lo), y: 4, z: 8, core: 2. Of those that a mesh axis runs over, the one named last changes fastest.
Arguments:
- prior_samples: bfloat16 [256, 128, 8192], P('mem', 'space'), may hold values from -6 to 6
- diffusivity_field: float32 [128, 8192], P('space'), may hold values from 0.05 to 0.24
- measured_site_position: int32 [8, 32, 512], P('space', 'mem'), may hold values from 0 to 4095
- measured_quantities: float32 [8, 32, 512], P('space', 'mem'), may hold values from -6 to 6
- measurement_weightings: float32 [8, 32, 512], P('space', 'mem'), may hold values from 0.5 to 8
Outputs:
- analysis: bfloat16 [256, 128, 8192], P('mem', 'space')
The draws below stay inside these ranges and needn't reach their ends.
Inputs may be any that keep to these rules, and one draw needn't show every extreme that they name: measured_site_position[p, q, o] names cell a * 256 + b of patch (p, q) itself.
All inputs are finite; a program needn't handle non-finite values.
Results may differ from the reference program's by a relative error of at most 0.0077.
Values may be sent and summed in bfloat16 or wider, within the bound.
No kernel may reach another device: no remote copies, remote signals or barrier semaphores. Data moves between devices by JAX's collectives and lax.ppermute only.
A program may use at most 64 MiB of HBM per device.

```python
import math
import jax
import jax.numpy as jnp
from jax import lax

SAMPLE_TOTAL = 256
A_DEV = 16
B_DEV = 256
OBS_DEV = 512
ITERS = 10
BLOCKS_A = 8
BLOCKS_B = 32
MESH_HEIGHT = 128
MESH_WIDTH = 8192


def with_ends(result, own_key, smallest, high):
    spot = [jax.random.randint(jax.random.fold_in(own_key, axis), (), 0, length) for axis, length in enumerate(result.shape)]
    longest = result.shape.index(max(result.shape))
    next_to = spot[:longest] + [(spot[longest] + 1) % result.shape[longest]] + spot[longest + 1:]
    return result.at[tuple(spot)].set(smallest).at[tuple(next_to)].set(high)


def steps_of(rng, dims, cuts, low, high):
    level, own = 1.0, jax.random.fold_in(rng, 6)
    for dim, shards_of in cuts:
        draws = jnp.exp(jax.random.uniform(jax.random.fold_in(own, dim), (shards_of,), jnp.float32, low / len(cuts), high / len(cuts)))
        level = level * jnp.repeat(draws, dims[dim] // shards_of).reshape([-1 if axis == dim else 1 for axis in range(len(dims))])
    return level


def scatter_about(stream_key, shape, scale, limit, split=(), kind=jnp.bfloat16):
    drawn = jax.random.normal(stream_key, shape, jnp.float32) * scale
    if len(split) > 0:
        drawn = steps_of(stream_key, shape, split, -0.22, 0.18) * drawn
    return jnp.clip(drawn, min=-limit, max=limit).astype(kind)


def setup_inputs(seed: int = 0) -> dict:
    arg_keys = jax.random.split(jax.random.key(seed), 6)
    prior_samples = scatter_about(arg_keys[0], (SAMPLE_TOTAL, MESH_HEIGHT, MESH_WIDTH), 1.0, 6.0, ((0, 32), (1, 8)))
    diffusivity_field = jnp.clip(0.05 + 0.19 * jax.random.uniform(arg_keys[1], (MESH_HEIGHT, MESH_WIDTH), jnp.float32) ** steps_of(arg_keys[1], (MESH_HEIGHT, MESH_WIDTH), ((0, 8),), -0.2, 0.2), 0.05, 0.24)
    measured_site_position = with_ends(jax.random.randint(arg_keys[2], (BLOCKS_A, BLOCKS_B, OBS_DEV), 0, A_DEV * B_DEV), jax.random.fold_in(arg_keys[2], 1), 0, (A_DEV * B_DEV) - 1).astype(jnp.int32)
    measured_quantities = scatter_about(arg_keys[3], (BLOCKS_A, BLOCKS_B, OBS_DEV), 1.0, 6.0, ((0, 8), (1, 32)), jnp.float32)
    measurement_weightings = jnp.clip(jnp.exp(math.log(8.0) - 2.7725887 * jax.random.uniform(arg_keys[4], (BLOCKS_A, BLOCKS_B, OBS_DEV), jnp.float32) ** steps_of(arg_keys[4], (BLOCKS_A, BLOCKS_B, OBS_DEV), ((0, 8), (1, 32)), -0.2, 0.2)), 0.5, 8.0)
    return {"prior_samples": prior_samples, "diffusivity_field": diffusivity_field, "measured_site_position": measured_site_position, "measured_quantities": measured_quantities, "measurement_weightings": measurement_weightings}


LOCALITY = ((0.25, 0.5, 0.25), (0.5, 1.0, 0.5), (0.25, 0.5, 0.25))
HIGHEST = lax.Precision.HIGHEST

def laplace(grid):
    padded = jnp.pad(grid, ((1, 1), (1, 1)))
    return padded[2:, 1:-1] + padded[:-2, 1:-1] + padded[1:-1, 2:] + padded[1:-1, :-2] - 4.0 * grid

def advance_prior(sample_label, diffusivity_field):
    present_sample = sample_label.astype(jnp.float32)
    present_sample = present_sample + diffusivity_field * laplace(present_sample)
    present_sample = present_sample + diffusivity_field * laplace(present_sample)
    return present_sample.astype(jnp.bfloat16)

def finish(sample_label, diffusivity_field):
    present_sample = sample_label.astype(jnp.float32)
    return (present_sample + diffusivity_field * laplace(present_sample)).astype(jnp.bfloat16)

def observe(patch_cells, indices, values, obs_weight):
    observed = jnp.take(patch_cells, indices, axis=1).astype(jnp.float32)
    obs_mean = lax.optimization_barrier(jnp.mean(observed, axis=0))
    obs_root = jnp.sqrt(obs_weight)
    spread = ((observed - obs_mean[None, :]) * obs_root[None, :]).astype(jnp.bfloat16)
    innovation = ((values - obs_mean) * obs_root).astype(jnp.bfloat16)
    spread_full = spread.astype(jnp.float32)
    own_gram = jnp.dot(spread_full, spread_full.T, precision=HIGHEST)
    own_vector = jnp.dot(spread_full, innovation.astype(jnp.float32), precision=HIGHEST)
    return (own_gram, own_vector)

def analyse(patch_cells, gram, vector):
    identity = jnp.eye(SAMPLE_TOTAL, dtype=jnp.float32)
    system = gram + (SAMPLE_TOTAL - 1.0) * identity
    frobenius = jnp.sqrt(jnp.sum(system * system))

    def newton(counter, pair):
        root_part, inverse_part = pair
        factor = 1.5 * identity - 0.5 * jnp.dot(inverse_part, root_part, precision=HIGHEST)
        return (jnp.dot(root_part, factor, precision=HIGHEST), jnp.dot(factor, inverse_part, precision=HIGHEST))
    root_part, inverse_part = lax.fori_loop(0, ITERS, newton, (system / frobenius, identity))
    inverse_root = inverse_part / jnp.sqrt(frobenius)
    mean_weights = jnp.dot(inverse_root, jnp.dot(inverse_root, vector, precision=HIGHEST), precision=HIGHEST)
    transform = (jnp.sqrt(SAMPLE_TOTAL - 1.0) * inverse_root + mean_weights[:, None]).astype(jnp.bfloat16)
    cells_full = patch_cells.astype(jnp.float32)
    state_mean = lax.optimization_barrier(jnp.mean(cells_full, axis=0))
    deviation = (cells_full - state_mean[None, :]).astype(jnp.bfloat16)
    moved = jnp.dot(transform.astype(jnp.float32).T, deviation.astype(jnp.float32), precision=HIGHEST)
    return (state_mean[None, :] + moved).astype(jnp.bfloat16)

def reference(prior_samples, diffusivity_field, measured_site_position, measured_quantities, measurement_weightings):
    advanced_sample = lax.map(lambda sample_label: advance_prior(sample_label, diffusivity_field), prior_samples)
    patches = advanced_sample.reshape(SAMPLE_TOTAL, BLOCKS_A, A_DEV, BLOCKS_B, B_DEV).transpose(1, 3, 0, 2, 4)
    patches = patches.reshape(BLOCKS_A, BLOCKS_B, SAMPLE_TOTAL, A_DEV * B_DEV)
    own_grams, own_vectors = lax.map(lambda group: jax.vmap(observe)(*group), (patches, measured_site_position, measured_quantities, measurement_weightings))
    padded_grams = jnp.pad(own_grams, ((1, 1), (1, 1), (0, 0), (0, 0)))
    padded_vectors = jnp.pad(own_vectors, ((1, 1), (1, 1), (0, 0)))
    gram = jnp.zeros_like(own_grams)
    vector = jnp.zeros_like(own_vectors)
    for first in range(3):
        for second in range(3):
            gram = gram + LOCALITY[first][second] * padded_grams[first:first + BLOCKS_A, second:second + BLOCKS_B]
            vector = vector + LOCALITY[first][second] * padded_vectors[first:first + BLOCKS_A, second:second + BLOCKS_B]
    updated = lax.map(lambda group: jax.vmap(analyse)(*group), (patches, gram, vector))
    updated = updated.reshape(BLOCKS_A, BLOCKS_B, SAMPLE_TOTAL, A_DEV, B_DEV).transpose(2, 0, 3, 1, 4).reshape(SAMPLE_TOTAL, MESH_HEIGHT, MESH_WIDTH)
    return lax.map(lambda sample_label: finish(sample_label, diffusivity_field), updated)
```

```python
import jax
import jax.numpy as jnp
from jax import lax
from jax.experimental import pallas as pl
from jax.experimental.pallas import tpu as pltpu
from jax.sharding import Mesh
from jax.sharding import PartitionSpec as P

ITERS = 10
MEM = ("mem_0", "mem_1", "mem_2")
F32 = jnp.float32
BF16 = jnp.bfloat16
VMEM_LIMIT = 48 << 20


def params():
    return pltpu.CompilerParams(vmem_limit_bytes=VMEM_LIMIT)


def vmem_specs(count):
    return [pl.BlockSpec(memory_space=pltpu.VMEM) for _ in range(count)]


def sides(window):
    width = window.shape[1]
    both = pltpu.roll(window, 1, axis=1) + pltpu.roll(window, width - 1, axis=1)
    return both[:, 128 : width - 128]


def forecast_kernel(x_ref, top_ref, bot_ref, coef_ref, out_ref, v1_ref):
    rows, _, width = x_ref.shape
    patches = out_ref.shape[0]
    cols = width // patches

    def source(r, off, size):
        if r < 0:
            piece = top_ref[r + 2, :, pl.ds(off, size)]
        elif r >= rows:
            piece = bot_ref[r - rows, :, pl.ds(off, size)]
        else:
            piece = x_ref[r, :, pl.ds(off, size)]
        return piece.astype(F32)

    def offsets(q):
        off = pl.multiple_of(q * cols, cols)
        before = pl.multiple_of(jnp.maximum(off - 128, 0), 128)
        after = pl.multiple_of(jnp.minimum(off + cols, width - 128), 128)
        return off, before, after

    def window(load, q):
        off, before, after = offsets(q)
        left = jnp.where(q > 0, load(before, 128), 0.0)
        right = jnp.where(q < patches - 1, load(after, 128), 0.0)
        return jnp.concatenate([left, load(off, cols), right], axis=1)

    def first(q, carry):
        off, _, _ = offsets(q)
        for e in range(rows + 2):
            r = e - 1
            wide = window(lambda o, s: source(r, o, s), q)
            mid = wide[:, 128 : 128 + cols]
            lap = source(r - 1, off, cols) + source(r + 1, off, cols) + sides(wide) - 4.0 * mid
            v1_ref[e, :, pl.ds(off, cols)] = mid + coef_ref[e : e + 1, pl.ds(off, cols)] * lap
        return carry

    def second(q, carry):
        off, _, _ = offsets(q)
        for a in range(rows):
            e = a + 1
            wide = window(lambda o, s: v1_ref[e, :, pl.ds(o, s)], q)
            mid = wide[:, 128 : 128 + cols]
            lap = (
                v1_ref[e - 1, :, pl.ds(off, cols)]
                + v1_ref[e + 1, :, pl.ds(off, cols)]
                + sides(wide)
                - 4.0 * mid
            )
            fresh = mid + coef_ref[e : e + 1, pl.ds(off, cols)] * lap
            out_ref[q, :, a * cols : (a + 1) * cols] = fresh.astype(BF16)
        return carry

    lax.fori_loop(0, patches, first, 0)
    lax.fori_loop(0, patches, second, 0)


def forecast(x, top, bot, coef, patches):
    rows, members, width = x.shape
    return pl.pallas_call(
        forecast_kernel,
        out_shape=jax.ShapeDtypeStruct((patches, members, rows * width // patches), BF16),
        in_specs=vmem_specs(4),
        out_specs=pl.BlockSpec(memory_space=pltpu.VMEM),
        scratch_shapes=[pltpu.VMEM((rows + 2, members, width), F32)],
        compiler_params=params(),
        name="forecast",
    )(x, top, bot, coef)


def observe_kernel(block_ref, site_ref, out_ref, *, cols):
    patches, members, cells = block_ref.shape
    count = site_ref.shape[1]
    rows = cells // cols

    def one(q, carry):
        site = site_ref[pl.ds(q, 1), :]
        row = lax.shift_right_logical(site, cols.bit_length() - 1)
        col = lax.bitwise_and(site, cols - 1)
        lanes = lax.broadcasted_iota(jnp.int32, (cols, count), 0)
        chosen = jnp.where(lanes == col, 1.0, 0.0).astype(BF16)
        stacked = jnp.concatenate(
            [block_ref[q, :, a * cols : (a + 1) * cols].astype(F32) for a in range(rows)], axis=0
        ).astype(BF16)
        picked = jnp.dot(stacked, chosen, preferred_element_type=F32)
        total = jnp.zeros((members, count), F32)
        for a in range(rows):
            total = jnp.where(row == a, picked[a * members : (a + 1) * members, :], total)
        out_ref[q, :, :] = total.astype(BF16)
        return carry

    lax.fori_loop(0, patches, one, 0)


def observe(blocks, sites, cols):
    patches, members, _ = blocks.shape
    return pl.pallas_call(
        lambda *refs: observe_kernel(*refs, cols=cols),
        out_shape=jax.ShapeDtypeStruct((patches, members, sites.shape[1]), BF16),
        in_specs=vmem_specs(2),
        out_specs=pl.BlockSpec(memory_space=pltpu.VMEM),
        compiler_params=params(),
        name="observe",
    )(blocks, sites)


def gram_kernel(obs_ref, value_ref, weight_ref, out_ref):
    groups, each, count = obs_ref.shape
    members = groups * each
    observed = obs_ref[...].astype(F32).reshape(members, count)
    mean = jnp.sum(observed, axis=0, keepdims=True) * (1.0 / members)
    root = jnp.sqrt(weight_ref[...])
    spread = ((observed - mean) * root).astype(BF16)
    innovation = ((value_ref[...] - mean) * root).astype(BF16)
    tail = jnp.broadcast_to(innovation.astype(F32), (16, count)).astype(BF16)
    left = jnp.concatenate([spread, tail], axis=0)
    both = lax.dot_general(left, spread, (((1,), (1,)), ((), ())), preferred_element_type=F32)
    out_ref[...] = both[: members + 8]


def gram_of(obs, values, weights):
    members = obs.shape[0] * obs.shape[1]
    return pl.pallas_call(
        gram_kernel,
        out_shape=jax.ShapeDtypeStruct((members + 8, members), F32),
        in_specs=vmem_specs(3),
        out_specs=pl.BlockSpec(memory_space=pltpu.VMEM),
        compiler_params=params(),
        name="gram",
    )(obs, values, weights)


def halves(value):
    high = value.astype(BF16)
    return high, (value - high.astype(F32)).astype(BF16)


def product(left, right):
    lh, ll = left
    rh, rl = right
    return (
        jnp.dot(lh, rh, preferred_element_type=F32)
        + jnp.dot(lh, rl, preferred_element_type=F32)
        + jnp.dot(ll, rh, preferred_element_type=F32)
    )


def root_kernel(low_ref, mid_ref, high_ref, out_ref):
    members = out_ref.shape[0]
    gram = 0.5 * low_ref[...] + mid_ref[...] + 0.5 * high_ref[...]
    vector = gram[members : members + 8]
    across = lax.broadcasted_iota(jnp.int32, (members, members), 0)
    along = lax.broadcasted_iota(jnp.int32, (members, members), 1)
    identity = jnp.where(across == along, 1.0, 0.0)
    system = gram[:members] + (members - 1.0) * identity
    squares = jnp.sum(jnp.sum(system * system, axis=0, keepdims=True), axis=1, keepdims=True)
    frob = jnp.sqrt(squares)
    root = system / frob
    factor = 1.5 * identity - 0.5 * root
    inverse = factor
    root = product(halves(root), halves(factor))
    for step in range(1, ITERS):
        root_h = halves(root)
        inverse_h = halves(inverse)
        factor_h = halves(1.5 * identity - 0.5 * product(inverse_h, root_h))
        if step < ITERS - 1:
            root = product(root_h, factor_h)
        inverse = product(factor_h, inverse_h)
    inverse_h = halves(inverse)
    weights = product(halves(product(halves(vector), inverse_h)), inverse_h) / frob
    scale = jnp.sqrt(members - 1.0) * lax.rsqrt(frob)
    out_ref[...] = (scale * inverse + weights[0:1]).astype(BF16)


def root_of(low, mid, high):
    members = mid.shape[1]
    return pl.pallas_call(
        root_kernel,
        out_shape=jax.ShapeDtypeStruct((members, members), BF16),
        in_specs=vmem_specs(3),
        out_specs=pl.BlockSpec(memory_space=pltpu.VMEM),
        compiler_params=params(),
        name="root",
    )(low, mid, high)


def update_kernel(turned_ref, block_ref, out_ref):
    groups, each, cells = block_ref.shape
    members = groups * each
    step = 512

    def one(c, carry):
        where = pl.ds(pl.multiple_of(c * step, step), step)
        cellwise = block_ref[:, :, where].astype(F32).reshape(members, step)
        mean = jnp.sum(cellwise, axis=0, keepdims=True) * (1.0 / members)
        deviation = (cellwise - mean).astype(BF16)
        moved = jnp.dot(turned_ref[...], deviation, preferred_element_type=F32)
        out_ref[:, :, where] = (mean + moved).reshape(groups, each, step).astype(BF16)
        return carry

    lax.fori_loop(0, cells // step, one, 0)


def update(turned, blocks):
    return pl.pallas_call(
        update_kernel,
        out_shape=jax.ShapeDtypeStruct(blocks.shape, BF16),
        in_specs=vmem_specs(2),
        out_specs=pl.BlockSpec(memory_space=pltpu.VMEM),
        compiler_params=params(),
        name="update",
    )(turned, blocks)


def finish_kernel(block_ref, top_ref, bot_ref, coef_ref, out_ref):
    patches, _, _ = block_ref.shape
    rows, _, width = out_ref.shape
    cols = width // patches

    def one(q, carry):
        off = pl.multiple_of(q * cols, cols)
        before = jnp.maximum(q - 1, 0)
        after = jnp.minimum(q + 1, patches - 1)
        mids = [top_ref[q].astype(F32)]
        for a in range(rows):
            mids.append(block_ref[q, :, a * cols : (a + 1) * cols].astype(F32))
        mids.append(bot_ref[q].astype(F32))
        for a in range(rows):
            left = block_ref[before, :, (a + 1) * cols - 128 : (a + 1) * cols].astype(F32)
            right = block_ref[after, :, a * cols : a * cols + 128].astype(F32)
            left = jnp.where(q > 0, left, 0.0)
            right = jnp.where(q < patches - 1, right, 0.0)
            mid = mids[a + 1]
            wide = jnp.concatenate([left, mid, right], axis=1)
            lap = mids[a] + mids[a + 2] + sides(wide) - 4.0 * mid
            done = mid + coef_ref[a : a + 1, pl.ds(off, cols)] * lap
            out_ref[a, :, pl.ds(off, cols)] = done.astype(BF16)
        return carry

    lax.fori_loop(0, patches, one, 0)


def finish(blocks, top, bot, coef):
    _, members, _ = blocks.shape
    rows, width = coef.shape
    return pl.pallas_call(
        finish_kernel,
        out_shape=jax.ShapeDtypeStruct((rows, members, width), BF16),
        in_specs=vmem_specs(4),
        out_specs=pl.BlockSpec(memory_space=pltpu.VMEM),
        compiler_params=params(),
        name="finish",
    )(blocks, top, bot, coef)


def from_both(axis, low_part, high_part):
    count = lax.axis_size(axis)
    forward = [(i, i + 1) for i in range(count - 1)]
    backward = [(i + 1, i) for i in range(count - 1)]
    return lax.ppermute(low_part, axis, forward), lax.ppermute(high_part, axis, backward)


def body(
    prior_samples,
    diffusivity_field,
    measured_site_position,
    measured_quantities,
    measurement_weightings,
):
    _, _, width = prior_samples.shape
    patches = lax.axis_size(MEM)
    cols = width // patches
    coef_low, coef_high = from_both("space", diffusivity_field[-1:], diffusivity_field[:1])
    top, bot = from_both(
        "space", jnp.swapaxes(prior_samples[:, -2:], 0, 1), jnp.swapaxes(prior_samples[:, :2], 0, 1)
    )
    sites = lax.all_to_all(
        jnp.broadcast_to(measured_site_position[0], (patches, measured_site_position.shape[2])),
        MEM, 0, 0, tiled=True,
    )
    coef = jnp.concatenate([coef_low, diffusivity_field, coef_high], axis=0)
    blocks = forecast(jnp.swapaxes(prior_samples, 0, 1), top, bot, coef, patches)
    obs = lax.all_to_all(observe(blocks, sites, cols), MEM, 0, 0, tiled=True)
    gathered = lax.all_to_all(blocks, MEM, 0, 0, tiled=True)
    own = gram_of(obs, measured_quantities[0], measurement_weightings[0])
    low, high = from_both(MEM, own, own)
    band = 0.5 * low + own + 0.5 * high
    low, high = from_both("space", band, band)
    turned = root_of(low, band, high)
    updated = update(turned, gathered)
    returned = lax.all_to_all(updated, MEM, 0, 0, tiled=True)
    top, bot = from_both("space", returned[:, :, -cols:], returned[:, :, :cols])
    done = finish(returned, top, bot, diffusivity_field)
    return jnp.swapaxes(done, 0, 1)


def solution(mesh):
    finer = Mesh(
        mesh.devices.reshape(2, 8, 2, mesh.shape["space"]), ("mem_0", "mem_1", "mem_2", "space")
    )
    in_specs = (
        P(MEM, "space", None),
        P("space", None),
        P("space", MEM, None),
        P("space", MEM, None),
        P("space", MEM, None),
    )
    out_specs = P(MEM, "space", None)
    return jax.shard_map(body, mesh=finer, in_specs=in_specs, out_specs=out_specs, check_vma=False)
```

```python
import jax
import jax.numpy as jnp
from jax import lax
from jax.experimental import pallas as pl
from jax.experimental.pallas import tpu as pltpu
from jax.sharding import Mesh
from jax.sharding import PartitionSpec as P

ITERS = 10
MEM = ("mem_0", "mem_1", "mem_2")
F32 = jnp.float32
BF16 = jnp.bfloat16
VMEM_LIMIT = 48 << 20


def params():
    return pltpu.CompilerParams(vmem_limit_bytes=VMEM_LIMIT)


def vmem_specs(count):
    return [pl.BlockSpec(memory_space=pltpu.VMEM) for _ in range(count)]


def sides(window):
    width = window.shape[1]
    both = pltpu.roll(window, 1, axis=1) + pltpu.roll(window, width - 1, axis=1)
    return both[:, 128 : width - 128]


def sweep(load, coef_ref, put, first, count, shift, off, width):
    above = load(first - 1)[:, 128 : 128 + width]
    here = load(first)
    for r in range(first, first + count):
        below = load(r + 1)
        mid = here[:, 128 : 128 + width]
        lap = (above + below[:, 128 : 128 + width]) + sides(here) - 4.0 * mid
        put(r, mid + coef_ref[r + shift : r + shift + 1, pl.ds(off, width)] * lap)
        above, here = mid, below


def edges_of(index, width, total):
    off = pl.multiple_of(index * width, width)
    before = pl.multiple_of(jnp.maximum(off - 128, 0), 128)
    after = pl.multiple_of(jnp.minimum(off + width, total - 128), 128)
    return off, before, after


def framed(left, mid, right, index, count):
    left = jnp.where(index > 0, left, 0.0)
    right = jnp.where(index < count - 1, right, 0.0)
    return jnp.concatenate([left, mid, right], axis=1)


CHUNK = 512


def forecast_kernel(x_ref, low_ref, high_ref, field_ref, out_ref, v1_ref, coef_ref):
    rows, _, width = x_ref.shape
    patches = out_ref.shape[0]
    cols = width // patches
    chunks = width // CHUNK
    coef_ref[pl.ds(8, rows), :] = field_ref[...]
    for ref, at in ((low_ref, 7), (high_ref, 8 + rows)):
        parts = ref[2].astype(F32)
        coef_ref[at : at + 1, :] = parts[0:1] + parts[1:2] + parts[2:3]

    def first(c, carry):
        off, before, after = edges_of(c, CHUNK, width)

        def load(r):
            ref, at = x_ref, r
            if r < 0:
                ref, at = low_ref, r + 2
            elif r >= rows:
                ref, at = high_ref, r - rows
            pieces = [ref[at, :, pl.ds(o, s)].astype(F32) for o, s in ((before, 128), (off, CHUNK), (after, 128))]
            return framed(*pieces, c, chunks)

        def put(r, value):
            v1_ref[r + 1, :, pl.ds(off, CHUNK)] = value

        sweep(load, coef_ref, put, -1, rows + 2, 8, off, CHUNK)
        return carry

    def second(c, carry):
        off, before, after = edges_of(c, CHUNK, width)

        def load(r):
            pieces = [v1_ref[r + 1, :, pl.ds(o, s)] for o, s in ((before, 128), (off, CHUNK), (after, 128))]
            return framed(*pieces, c, chunks)

        def put(r, value):
            for k in range(CHUNK // cols):
                out_ref[c * (CHUNK // cols) + k, :, r * cols : (r + 1) * cols] = value[
                    :, k * cols : (k + 1) * cols
                ].astype(BF16)

        sweep(load, coef_ref, put, 0, rows, 8, off, CHUNK)
        return carry

    lax.fori_loop(0, chunks, first, 0)
    lax.fori_loop(0, chunks, second, 0)


def forecast(x, low, high, field, patches):
    rows, members, width = x.shape
    return pl.pallas_call(
        forecast_kernel,
        out_shape=jax.ShapeDtypeStruct((patches, members, rows * width // patches), BF16),
        in_specs=vmem_specs(4),
        out_specs=pl.BlockSpec(memory_space=pltpu.VMEM),
        scratch_shapes=[pltpu.VMEM((rows + 2, members, width), F32), pltpu.VMEM((rows + 16, width), F32)],
        compiler_params=params(),
        name="forecast",
    )(x, low, high, field)


def gram_kernel(block_ref, site_ref, value_ref, weight_ref, out_ref):
    groups, each, cells = block_ref.shape
    members = groups * each
    count = site_ref.shape[1]
    half = members // 2
    step = 512
    site = site_ref[...]
    observed = jnp.zeros((members, count), F32)
    for c in range(cells // step):
        cell = lax.broadcasted_iota(jnp.int32, (step, count), 0) + c * step
        chosen = jnp.where(cell == site, 1.0, 0.0).astype(BF16)
        piece = block_ref[:, :, c * step : (c + 1) * step].reshape(members, step)
        observed += jnp.dot(piece, chosen, preferred_element_type=F32)
    mean = jnp.sum(observed, axis=0, keepdims=True) * (1.0 / members)
    root = jnp.sqrt(weight_ref[...])
    spread = ((observed - mean) * root).astype(BF16)
    innovation = ((value_ref[...] - mean) * root).astype(BF16)
    tail = jnp.broadcast_to(innovation.astype(F32), (16, count)).astype(BF16)
    left = jnp.concatenate([spread, tail], axis=0)
    both = lax.dot_general(left, spread, (((1,), (1,)), ((), ())), preferred_element_type=F32)
    low = both[half:members, half:]
    across = lax.broadcasted_iota(jnp.int32, (half, half), 0)
    along = lax.broadcasted_iota(jnp.int32, (half, half), 1)
    corner = jnp.sum(jnp.where(across == along, low, 0.0), axis=0, keepdims=True)
    out_ref[:half, :half] = jnp.where(across <= along, both[:half, :half], low)
    out_ref[:half, half:] = both[:half, half:]
    out_ref[half:, :] = both[members : members + 8]
    out_ref[half + 1 : half + 2, :half] = corner


def gram_of(blocks, sites, values, weights):
    members = blocks.shape[0] * blocks.shape[1]
    return pl.pallas_call(
        gram_kernel,
        out_shape=jax.ShapeDtypeStruct((members // 2 + 8, members), F32),
        in_specs=vmem_specs(4),
        out_specs=pl.BlockSpec(memory_space=pltpu.VMEM),
        compiler_params=params(),
        name="gram",
    )(blocks, sites, values, weights)


def unpacked(packed, half):
    across = lax.broadcasted_iota(jnp.int32, (half, half), 0)
    along = lax.broadcasted_iota(jnp.int32, (half, half), 1)
    block = packed[:half, :half]
    turned = block.T
    upper = jnp.where(across <= along, block, turned)
    lower = jnp.where(across > along, block, turned)
    lower = jnp.where(across == along, packed[half + 1 : half + 2, :half], lower)
    side = packed[:half, half:]
    return jnp.concatenate(
        [jnp.concatenate([upper, side], axis=1), jnp.concatenate([side.T, lower], axis=1)], axis=0
    )


def halves(value):
    high = value.astype(BF16)
    return high, (value - high.astype(F32)).astype(BF16)


def product(left, right):
    lh, ll = left
    rh, rl = right
    return (
        jnp.dot(lh, rh, preferred_element_type=F32)
        + jnp.dot(lh, rl, preferred_element_type=F32)
        + jnp.dot(ll, rh, preferred_element_type=F32)
    )


def root_kernel(low_ref, mid_ref, high_ref, out_ref):
    members = out_ref.shape[0]
    half = members // 2
    packed = 0.5 * low_ref[...] + mid_ref[...] + 0.5 * high_ref[...]
    vector = packed[half : half + 8]
    gram = unpacked(packed, half)
    across = lax.broadcasted_iota(jnp.int32, (members, members), 0)
    along = lax.broadcasted_iota(jnp.int32, (members, members), 1)
    identity = jnp.where(across == along, 1.0, 0.0)
    system = gram + (members - 1.0) * identity
    squares = jnp.sum(jnp.sum(system * system, axis=0, keepdims=True), axis=1, keepdims=True)
    frob = jnp.sqrt(squares)
    root = system / frob
    factor = 1.5 * identity - 0.5 * root
    inverse = factor
    root = product(halves(root), halves(factor))
    for step in range(1, ITERS):
        root_h = halves(root)
        inverse_h = halves(inverse)
        factor_h = halves(1.5 * identity - 0.5 * product(inverse_h, root_h))
        if step < ITERS - 1:
            root = product(root_h, factor_h)
        inverse = product(factor_h, inverse_h)
    inverse_h = halves(inverse)
    weights = product(halves(product(halves(vector), inverse_h)), inverse_h) / frob
    scale = jnp.sqrt(members - 1.0) * lax.rsqrt(frob)
    out_ref[...] = (scale * inverse + weights[0:1]).astype(BF16)


def root_of(low, mid, high):
    members = mid.shape[1]
    return pl.pallas_call(
        root_kernel,
        out_shape=jax.ShapeDtypeStruct((members, members), BF16),
        in_specs=vmem_specs(3),
        out_specs=pl.BlockSpec(memory_space=pltpu.VMEM),
        compiler_params=params(),
        name="root",
    )(low, mid, high)


def center_kernel(block_ref, mean_ref, out_ref):
    groups, each, cells = block_ref.shape
    members = groups * each
    step = 256

    def one(c, carry):
        where = pl.ds(pl.multiple_of(c * step, step), step)
        cellwise = block_ref[:, :, where].astype(F32)
        mean = jnp.sum(jnp.sum(cellwise, axis=0), axis=0, keepdims=True) * (1.0 / members)
        mean_ref[:, where] = mean
        out_ref[:, where] = (cellwise.reshape(members, step) - mean).astype(BF16)
        return carry

    lax.fori_loop(0, cells // step, one, 0)


def centered(blocks):
    groups, each, cells = blocks.shape
    return pl.pallas_call(
        center_kernel,
        out_shape=(
            jax.ShapeDtypeStruct((1, cells), F32),
            jax.ShapeDtypeStruct((groups * each, cells), BF16),
        ),
        in_specs=vmem_specs(1),
        out_specs=tuple(vmem_specs(2)),
        compiler_params=params(),
        name="center",
    )(blocks)


def update_kernel(turned_ref, mean_ref, deviation_ref, out_ref):
    groups, each, cells = out_ref.shape
    step = 512

    def one(c, carry):
        where = pl.ds(pl.multiple_of(c * step, step), step)
        moved = jnp.dot(turned_ref[...], deviation_ref[:, where], preferred_element_type=F32)
        out_ref[:, :, where] = (mean_ref[:, where] + moved).reshape(groups, each, step).astype(BF16)
        return carry

    lax.fori_loop(0, cells // step, one, 0)


def update(turned, mean, deviation, shape):
    return pl.pallas_call(
        update_kernel,
        out_shape=jax.ShapeDtypeStruct(shape, BF16),
        in_specs=vmem_specs(3),
        out_specs=pl.BlockSpec(memory_space=pltpu.VMEM),
        compiler_params=params(),
        name="update",
    )(turned, mean, deviation)


def finish_kernel(block_ref, low_ref, high_ref, coef_ref, out_ref):
    patches, _, _ = block_ref.shape
    rows, _, width = out_ref.shape
    cols = width // patches
    chunks = width // CHUNK
    each = CHUNK // cols

    def one(c, carry):
        off = pl.multiple_of(c * CHUNK, CHUNK)
        base = c * each
        before = jnp.maximum(base - 1, 0)
        after = jnp.minimum(base + each, patches - 1)

        def load(r):
            ref, at = block_ref, r * cols
            if r < 0:
                ref, at = low_ref, 0
            elif r >= rows:
                ref, at = high_ref, 0
            pieces = [ref[before, :, at + cols - 128 : at + cols]]
            pieces += [ref[base + k, :, at : at + cols] for k in range(each)]
            pieces += [ref[after, :, at : at + 128]]
            pieces = [p.astype(F32) for p in pieces]
            return framed(pieces[0], jnp.concatenate(pieces[1:-1], axis=1), pieces[-1], c, chunks)

        def put(r, value):
            out_ref[r, :, pl.ds(off, CHUNK)] = value.astype(BF16)

        sweep(load, coef_ref, put, 0, rows, 0, off, CHUNK)
        return carry

    lax.fori_loop(0, chunks, one, 0)


def finish(blocks, top, bot, coef):
    _, members, _ = blocks.shape
    rows, width = coef.shape
    return pl.pallas_call(
        finish_kernel,
        out_shape=jax.ShapeDtypeStruct((rows, members, width), BF16),
        in_specs=vmem_specs(4),
        out_specs=pl.BlockSpec(memory_space=pltpu.VMEM),
        compiler_params=params(),
        name="finish",
    )(blocks, top, bot, coef)


def from_both(axis, to_next, to_previous):
    count = lax.axis_size(axis)
    forward = [(i, i + 1) for i in range(count - 1)]
    backward = [(i + 1, i) for i in range(count - 1)]
    return lax.ppermute(to_next, axis, forward), lax.ppermute(to_previous, axis, backward)


def in_three(row):
    high = lax.reduce_precision(row, 8, 7)
    middle = lax.reduce_precision(row - high, 8, 7)
    parts = jnp.concatenate([high, middle, row - high - middle], axis=0).astype(BF16)
    return jnp.pad(parts, ((0, 5), (0, 0)))[None]


def body(
    prior_samples,
    diffusivity_field,
    measured_site_position,
    measured_quantities,
    measurement_weightings,
):
    patches = lax.axis_size(MEM)
    cols = prior_samples.shape[2] // patches
    low, high = from_both(
        "space",
        jnp.concatenate(
            [jnp.swapaxes(prior_samples[:, -2:], 0, 1), in_three(diffusivity_field[-1:])], axis=0
        ),
        jnp.concatenate(
            [jnp.swapaxes(prior_samples[:, :2], 0, 1), in_three(diffusivity_field[:1])], axis=0
        ),
    )
    turned_prior = jnp.swapaxes(prior_samples, 0, 1)
    blocks = forecast(turned_prior, low, high, diffusivity_field, patches)
    gathered = lax.all_to_all(blocks, MEM, 0, 0, tiled=True)
    own = gram_of(
        gathered, measured_site_position[0], measured_quantities[0], measurement_weightings[0]
    )
    low, high = from_both(MEM, own, own)
    mean, deviation = centered(gathered)
    band = 0.5 * low + own + 0.5 * high
    low, high = from_both("space", band, band)
    updated = update(root_of(low, band, high), mean, deviation, gathered.shape)
    returned = lax.all_to_all(updated, MEM, 0, 0, tiled=True)
    low, high = from_both("space", returned[:, :, -cols:], returned[:, :, :cols])
    done = finish(returned, low, high, diffusivity_field)
    return jnp.swapaxes(done, 0, 1)


def solution(mesh):
    finer = Mesh(
        mesh.devices.reshape(2, 8, 2, mesh.shape["space"]), ("mem_0", "mem_1", "mem_2", "space")
    )
    in_specs = (
        P(MEM, "space", None),
        P("space", None),
        P("space", MEM, None),
        P("space", MEM, None),
        P("space", MEM, None),
    )
    out_specs = P(MEM, "space", None)
    return jax.shard_map(body, mesh=finer, in_specs=in_specs, out_specs=out_specs, check_vma=False)
```

```python
import jax
import jax.numpy as jnp
from jax import lax
from jax.experimental import pallas as pl
from jax.experimental.pallas import tpu as pltpu
from jax.sharding import Mesh
from jax.sharding import PartitionSpec as P

ITERS = 10
MEM = ("mem_0", "mem_1", "mem_2")
F32 = jnp.float32
BF16 = jnp.bfloat16
VMEM_LIMIT = 48 << 20


def params():
    return pltpu.CompilerParams(vmem_limit_bytes=VMEM_LIMIT)


def vmem_specs(count):
    return [pl.BlockSpec(memory_space=pltpu.VMEM) for _ in range(count)]


def sides(window):
    width = window.shape[1]
    both = pltpu.roll(window, 1, axis=1) + pltpu.roll(window, width - 1, axis=1)
    return both[:, 128 : width - 128]


def sweep(load, coef_ref, put, first, count, shift, off, width):
    above = load(first - 1)[:, 128 : 128 + width]
    here = load(first)
    for r in range(first, first + count):
        below = load(r + 1)
        mid = here[:, 128 : 128 + width]
        lap = (above + below[:, 128 : 128 + width]) + sides(here) - 4.0 * mid
        put(r, mid + coef_ref[r + shift : r + shift + 1, pl.ds(off, width)] * lap)
        above, here = mid, below


def edges_of(index, width, total):
    off = pl.multiple_of(index * width, width)
    before = pl.multiple_of(jnp.maximum(off - 128, 0), 128)
    after = pl.multiple_of(jnp.minimum(off + width, total - 128), 128)
    return off, before, after


def framed(left, mid, right, index, count):
    left = jnp.where(index > 0, left, 0.0)
    right = jnp.where(index < count - 1, right, 0.0)
    return jnp.concatenate([left, mid, right], axis=1)


CHUNK = 512


def ends_kernel(odd_ref, x_ref, field_ref, one_ref, two_ref):
    members, rows, width = x_ref.shape
    odd = odd_ref[0] > 0

    def put(where, low, high):
        one_ref[:, where] = jnp.where(odd, low, high).astype(BF16)
        two_ref[:, where] = jnp.where(odd, high, low).astype(BF16)

    def some(c, carry):
        off = pl.multiple_of(c * CHUNK, CHUNK)
        tall = [x_ref[m, :, pl.ds(off, CHUNK)].astype(F32) for m in range(members)]
        for k in range(2):
            low = jnp.concatenate([t[k : k + 1] for t in tall], axis=0)
            high = jnp.concatenate([t[rows - 2 + k : rows - 1 + k] for t in tall], axis=0)
            put(pl.ds(pl.multiple_of(k * width + off, CHUNK), CHUNK), low, high)
        return carry

    lax.fori_loop(0, width // CHUNK, some, 0)
    piece = width // members

    def folded(row):
        lines = [field_ref[row : row + 1, s * piece : (s + 1) * piece] for s in range(members)]
        whole = jnp.concatenate(lines, axis=0)
        high, rest = halves(whole)
        low = whole - high.astype(F32) - rest.astype(F32)
        return [high.astype(F32), rest.astype(F32), low]

    for k, (low, high) in enumerate(zip(folded(0), folded(rows - 1))):
        begin = 2 * width + k * piece
        put(slice(begin, begin + piece), low, high)


def ends(odd, x, field):
    members, _, width = x.shape
    shape = jax.ShapeDtypeStruct((members, 2 * width + 3 * width // members), BF16)
    return pl.pallas_call(
        ends_kernel,
        out_shape=(shape, shape),
        in_specs=[pl.BlockSpec(memory_space=pltpu.SMEM)] + vmem_specs(2),
        out_specs=tuple(vmem_specs(2)),
        compiler_params=params(),
        name="ends",
    )(odd, x, field)


def first_pass(source, coef_ref, v1_ref, index, width, spans, shift):
    off, before, after = edges_of(index, CHUNK, width)

    def load(r):
        pieces = [source(r, o, s) for o, s in ((before, 128), (off, CHUNK), (after, 128))]
        return framed(*pieces, index, width // CHUNK)

    for begin, count in spans:

        def put(r, value):
            v1_ref[r + 1, :, pl.ds(off, CHUNK)] = value

        sweep(load, coef_ref, put, begin, count, shift, off, CHUNK)


def second_pass(coef_ref, v1_ref, out_ref, index, width, spans, shift):
    cols = width // out_ref.shape[0]
    each = CHUNK // cols
    off, before, after = edges_of(index, CHUNK, width)

    def load(r):
        pieces = [v1_ref[r + 1, :, pl.ds(o, s)] for o, s in ((before, 128), (off, CHUNK), (after, 128))]
        return framed(*pieces, index, width // CHUNK)

    def put(r, value):
        for k in range(each):
            out_ref[index * each + k, :, r * cols : (r + 1) * cols] = value[
                :, k * cols : (k + 1) * cols
            ].astype(BF16)

    for begin, count in spans:
        sweep(load, coef_ref, put, begin, count, shift, off, CHUNK)


def inner_kernel(x_ref, field_ref, out_ref, v1_ref):
    rows, _, width = x_ref.shape

    def first(c, carry):
        def source(r, off, size):
            return x_ref[r, :, pl.ds(off, size)].astype(F32)

        first_pass(source, field_ref, v1_ref, c, width, ((1, rows - 2),), 0)
        return carry

    def second(c, carry):
        second_pass(field_ref, v1_ref, out_ref, c, width, ((2, rows - 4),), 0)
        return carry

    lax.fori_loop(0, width // CHUNK, first, 0)
    lax.fori_loop(0, width // CHUNK, second, 0)


def inner_forecast(x, field, patches):
    rows, members, width = x.shape
    return pl.pallas_call(
        inner_kernel,
        out_shape=jax.ShapeDtypeStruct((patches, members, rows * width // patches), BF16),
        in_specs=vmem_specs(2),
        out_specs=pl.BlockSpec(memory_space=pltpu.VMEM),
        scratch_shapes=[pltpu.VMEM((rows + 2, members, width), F32)],
        compiler_params=params(),
        name="inner",
    )(x, field)


def outer_kernel(odd_ref, x_ref, one_ref, two_ref, field_ref, part_ref, out_ref, v1_ref, coef_ref):
    rows, members, width = x_ref.shape
    del part_ref
    odd = odd_ref[0] > 0
    piece = width // members
    coef_ref[pl.ds(8, rows), :] = field_ref[...]
    one = one_ref[:, 2 * width :].astype(F32)
    two = two_ref[:, 2 * width :].astype(F32)
    one = one[:, :piece] + one[:, piece : 2 * piece] + one[:, 2 * piece :]
    two = two[:, :piece] + two[:, piece : 2 * piece] + two[:, 2 * piece :]
    low = jnp.where(odd, one, two)
    high = jnp.where(odd, two, one)
    for s in range(members):
        coef_ref[7:8, s * piece : (s + 1) * piece] = low[s : s + 1]
        coef_ref[8 + rows : 9 + rows, s * piece : (s + 1) * piece] = high[s : s + 1]

    def first(c, carry):
        def source(r, off, size):
            if 0 <= r < rows:
                return x_ref[r, :, pl.ds(off, size)].astype(F32)
            at = (r + 2 if r < 0 else r - rows) * width
            a = one_ref[:, pl.ds(at + off, size)].astype(F32)
            b = two_ref[:, pl.ds(at + off, size)].astype(F32)
            return jnp.where(odd, a, b) if r < 0 else jnp.where(odd, b, a)

        first_pass(source, coef_ref, v1_ref, c, width, ((-1, 4), (rows - 3, 4)), 8)
        return carry

    def second(c, carry):
        second_pass(coef_ref, v1_ref, out_ref, c, width, ((0, 2), (rows - 2, 2)), 8)
        return carry

    lax.fori_loop(0, width // CHUNK, first, 0)
    lax.fori_loop(0, width // CHUNK, second, 0)


def outer_forecast(odd, x, one, two, field, part):
    rows, members, width = x.shape
    return pl.pallas_call(
        outer_kernel,
        out_shape=jax.ShapeDtypeStruct(part.shape, BF16),
        in_specs=[pl.BlockSpec(memory_space=pltpu.SMEM)] + vmem_specs(5),
        out_specs=pl.BlockSpec(memory_space=pltpu.VMEM),
        scratch_shapes=[pltpu.VMEM((rows + 2, members, width), F32), pltpu.VMEM((rows + 16, width), F32)],
        input_output_aliases={5: 0},
        compiler_params=params(),
        name="outer",
    )(odd, x, one, two, field, part)


def gram_kernel(block_ref, site_ref, value_ref, weight_ref, out_ref):
    groups, each, cells = block_ref.shape
    members = groups * each
    count = site_ref.shape[1]
    half = members // 2
    step = 512
    site = site_ref[...]
    observed = jnp.zeros((members, count), F32)
    for c in range(cells // step):
        cell = lax.broadcasted_iota(jnp.int32, (step, count), 0) + c * step
        chosen = jnp.where(cell == site, 1.0, 0.0).astype(BF16)
        piece = block_ref[:, :, c * step : (c + 1) * step].reshape(members, step)
        observed += jnp.dot(piece, chosen, preferred_element_type=F32)
    mean = jnp.sum(observed, axis=0, keepdims=True) * (1.0 / members)
    root = jnp.sqrt(weight_ref[...])
    spread = ((observed - mean) * root).astype(BF16)
    innovation = ((value_ref[...] - mean) * root).astype(BF16)
    tail = jnp.broadcast_to(innovation.astype(F32), (16, count)).astype(BF16)
    left = jnp.concatenate([spread, tail], axis=0)
    both = lax.dot_general(left, spread, (((1,), (1,)), ((), ())), preferred_element_type=F32)
    low = both[half:members, half:]
    across = lax.broadcasted_iota(jnp.int32, (half, half), 0)
    along = lax.broadcasted_iota(jnp.int32, (half, half), 1)
    corner = jnp.sum(jnp.where(across == along, low, 0.0), axis=0, keepdims=True)
    out_ref[:half, :half] = jnp.where(across <= along, both[:half, :half], low)
    out_ref[:half, half:] = both[:half, half:]
    out_ref[half:, :] = both[members : members + 8]
    out_ref[half + 1 : half + 2, :half] = corner


def gram_of(blocks, sites, values, weights):
    members = blocks.shape[0] * blocks.shape[1]
    return pl.pallas_call(
        gram_kernel,
        out_shape=jax.ShapeDtypeStruct((members // 2 + 8, members), F32),
        in_specs=vmem_specs(4),
        out_specs=pl.BlockSpec(memory_space=pltpu.VMEM),
        compiler_params=params(),
        name="gram",
    )(blocks, sites, values, weights)


def unpacked(packed, half):
    across = lax.broadcasted_iota(jnp.int32, (half, half), 0)
    along = lax.broadcasted_iota(jnp.int32, (half, half), 1)
    block = packed[:half, :half]
    turned = block.T
    upper = jnp.where(across <= along, block, turned)
    lower = jnp.where(across > along, block, turned)
    lower = jnp.where(across == along, packed[half + 1 : half + 2, :half], lower)
    side = packed[:half, half:]
    return jnp.concatenate(
        [jnp.concatenate([upper, side], axis=1), jnp.concatenate([side.T, lower], axis=1)], axis=0
    )


def halves(value):
    high = value.astype(BF16)
    return high, (value - high.astype(F32)).astype(BF16)


def product(left, right):
    lh, ll = left
    rh, rl = right
    return (
        jnp.dot(lh, rh, preferred_element_type=F32)
        + jnp.dot(lh, rl, preferred_element_type=F32)
        + jnp.dot(ll, rh, preferred_element_type=F32)
    )


def root_kernel(one_ref, mid_ref, two_ref, out_ref):
    members = out_ref.shape[0]
    half = members // 2
    packed = mid_ref[...] + 0.5 * (one_ref[...] + two_ref[...])
    vector = packed[half : half + 8]
    gram = unpacked(packed, half)
    across = lax.broadcasted_iota(jnp.int32, (members, members), 0)
    along = lax.broadcasted_iota(jnp.int32, (members, members), 1)
    identity = jnp.where(across == along, 1.0, 0.0)
    system = gram + (members - 1.0) * identity
    squares = jnp.sum(jnp.sum(system * system, axis=0, keepdims=True), axis=1, keepdims=True)
    frob = jnp.sqrt(squares)
    root = system / frob
    factor = 1.5 * identity - 0.5 * root
    inverse = factor
    root = product(halves(root), halves(factor))
    for step in range(1, ITERS):
        root_h = halves(root)
        inverse_h = halves(inverse)
        factor_h = halves(1.5 * identity - 0.5 * product(inverse_h, root_h))
        if step < ITERS - 1:
            root = product(root_h, factor_h)
        inverse = product(factor_h, inverse_h)
    inverse_h = halves(inverse)
    weights = product(halves(product(halves(vector), inverse_h)), inverse_h) / frob
    scale = jnp.sqrt(members - 1.0) * lax.rsqrt(frob)
    out_ref[...] = (scale * inverse + weights[0:1]).astype(BF16)


def root_of(one, mid, two):
    members = mid.shape[1]
    return pl.pallas_call(
        root_kernel,
        out_shape=jax.ShapeDtypeStruct((members, members), BF16),
        in_specs=vmem_specs(3),
        out_specs=pl.BlockSpec(memory_space=pltpu.VMEM),
        compiler_params=params(),
        name="root",
    )(one, mid, two)


def center_kernel(block_ref, mean_ref, out_ref):
    groups, each, cells = block_ref.shape
    members = groups * each
    step = 256

    def one(c, carry):
        where = pl.ds(pl.multiple_of(c * step, step), step)
        cellwise = block_ref[:, :, where].astype(F32)
        mean = jnp.sum(jnp.sum(cellwise, axis=0), axis=0, keepdims=True) * (1.0 / members)
        mean_ref[:, where] = mean
        out_ref[:, where] = (cellwise.reshape(members, step) - mean).astype(BF16)
        return carry

    lax.fori_loop(0, cells // step, one, 0)


def centered(blocks):
    groups, each, cells = blocks.shape
    return pl.pallas_call(
        center_kernel,
        out_shape=(
            jax.ShapeDtypeStruct((1, cells), F32),
            jax.ShapeDtypeStruct((groups * each, cells), BF16),
        ),
        in_specs=vmem_specs(1),
        out_specs=tuple(vmem_specs(2)),
        compiler_params=params(),
        name="center",
    )(blocks)


def update_kernel(turned_ref, mean_ref, deviation_ref, out_ref):
    groups, each, cells = out_ref.shape
    step = 512

    def one(c, carry):
        where = pl.ds(pl.multiple_of(c * step, step), step)
        moved = jnp.dot(turned_ref[...], deviation_ref[:, where], preferred_element_type=F32)
        out_ref[:, :, where] = (mean_ref[:, where] + moved).reshape(groups, each, step).astype(BF16)
        return carry

    lax.fori_loop(0, cells // step, one, 0)


def update(turned, mean, deviation, shape):
    return pl.pallas_call(
        update_kernel,
        out_shape=jax.ShapeDtypeStruct(shape, BF16),
        in_specs=vmem_specs(3),
        out_specs=pl.BlockSpec(memory_space=pltpu.VMEM),
        compiler_params=params(),
        name="update",
    )(turned, mean, deviation)


def final_rows(source, coef_ref, out_ref, index, cols, patches, spans):
    each = CHUNK // cols
    base = index * each
    off = pl.multiple_of(index * CHUNK, CHUNK)
    before = jnp.maximum(base - 1, 0)
    after = jnp.minimum(base + each, patches - 1)

    def load(r):
        left = source(r, before, cols - 128, cols)
        mid = jnp.concatenate([source(r, base + k, 0, cols) for k in range(each)], axis=1)
        return framed(left, mid, source(r, after, 0, 128), index, patches // each)

    def put(r, value):
        out_ref[r, :, pl.ds(off, CHUNK)] = value.astype(BF16)

    for begin, count in spans:
        sweep(load, coef_ref, put, begin, count, 0, off, CHUNK)


def middle_kernel(block_ref, coef_ref, out_ref):
    patches, _, cells = block_ref.shape
    rows = coef_ref.shape[0]
    cols = cells // rows

    def one(c, carry):
        def source(r, q, begin, end):
            return block_ref[q, :, r * cols + begin : r * cols + end].astype(F32)

        final_rows(source, coef_ref, out_ref, c, cols, patches, ((1, rows - 2),))
        return carry

    lax.fori_loop(0, patches * cols // CHUNK, one, 0)


def middle_rows(blocks, coef):
    _, members, _ = blocks.shape
    rows, width = coef.shape
    return pl.pallas_call(
        middle_kernel,
        out_shape=jax.ShapeDtypeStruct((rows, members, width), BF16),
        in_specs=vmem_specs(2),
        out_specs=pl.BlockSpec(memory_space=pltpu.VMEM),
        compiler_params=params(),
        name="middle",
    )(blocks, coef)


def rim_kernel(odd_ref, block_ref, one_ref, two_ref, coef_ref, part_ref, out_ref):
    patches, _, cells = block_ref.shape
    rows = coef_ref.shape[0]
    cols = cells // rows
    odd = odd_ref[0] > 0
    del part_ref

    def one(c, carry):
        def source(r, q, begin, end):
            if 0 <= r < rows:
                return block_ref[q, :, r * cols + begin : r * cols + end].astype(F32)
            a = one_ref[q, :, begin:end].astype(F32)
            b = two_ref[q, :, begin:end].astype(F32)
            return jnp.where(odd, a, b) if r < 0 else jnp.where(odd, b, a)

        final_rows(source, coef_ref, out_ref, c, cols, patches, ((0, 1), (rows - 1, 1)))
        return carry

    lax.fori_loop(0, patches * cols // CHUNK, one, 0)


def rim_rows(odd, blocks, one, two, coef, part):
    return pl.pallas_call(
        rim_kernel,
        out_shape=jax.ShapeDtypeStruct(part.shape, BF16),
        in_specs=[pl.BlockSpec(memory_space=pltpu.SMEM)] + vmem_specs(5),
        out_specs=pl.BlockSpec(memory_space=pltpu.VMEM),
        input_output_aliases={5: 0},
        compiler_params=params(),
        name="rim",
    )(odd, blocks, one, two, coef, part)


def swaps(axis, in_one, in_two):
    count = lax.axis_size(axis)

    def pairs(first):
        both = [(i, i + 1) for i in range(first, count - 1, 2)]
        return both + [(j, i) for i, j in both]

    two = lax.ppermute(in_two, axis, pairs(1))
    one = lax.ppermute(in_one, axis, pairs(0))
    return one, two


def body(
    prior_samples,
    diffusivity_field,
    measured_site_position,
    measured_quantities,
    measurement_weightings,
):
    patches = lax.axis_size(MEM)
    _, _, width = prior_samples.shape
    cols = width // patches
    odd = lax.bitwise_and(lax.axis_index("space"), 1)
    flag = odd.reshape(1)
    one, two = swaps("space", *ends(flag, prior_samples, diffusivity_field))
    turned_prior = jnp.swapaxes(prior_samples, 0, 1)
    part = inner_forecast(turned_prior, diffusivity_field, patches)
    blocks = outer_forecast(flag, turned_prior, one, two, diffusivity_field, part)
    gathered = lax.all_to_all(blocks, MEM, 0, 0, tiled=True)
    own = gram_of(
        gathered, measured_site_position[0], measured_quantities[0], measurement_weightings[0]
    )
    one, two = swaps(MEM, own, own)
    mean, deviation = centered(gathered)
    band = own + 0.5 * (one + two)
    one, two = swaps("space", band, band)
    updated = update(root_of(one, band, two), mean, deviation, gathered.shape)
    returned = lax.all_to_all(updated, MEM, 0, 0, tiled=True)
    last, start = returned[:, :, -cols:], returned[:, :, :cols]
    one, two = swaps("space", jnp.where(odd > 0, start, last), jnp.where(odd > 0, last, start))
    part = middle_rows(returned, diffusivity_field)
    done = rim_rows(flag, returned, one, two, diffusivity_field, part)
    return jnp.swapaxes(done, 0, 1)


def solution(mesh):
    finer = Mesh(
        mesh.devices.reshape(2, 8, 2, mesh.shape["space"]), ("mem_0", "mem_1", "mem_2", "space")
    )
    in_specs = (
        P(MEM, "space", None),
        P("space", None),
        P("space", MEM, None),
        P("space", MEM, None),
        P("space", MEM, None),
    )
    out_specs = P(MEM, "space", None)
    return jax.shard_map(body, mesh=finer, in_specs=in_specs, out_specs=out_specs, check_vma=False)
```

```python
import jax
import jax.numpy as jnp
from jax import lax
from jax.experimental import pallas as pl
from jax.experimental.pallas import tpu as pltpu
from jax.sharding import Mesh
from jax.sharding import PartitionSpec as P

ITERS = 10
MEM = ("mem_0", "mem_1", "mem_2")
F32 = jnp.float32
BF16 = jnp.bfloat16
VMEM_LIMIT = 48 << 20


def params():
    return pltpu.CompilerParams(vmem_limit_bytes=VMEM_LIMIT)


def is_odd():
    return lax.bitwise_and(lax.axis_index("space"), 1) > 0


def vmem_specs(count):
    return [pl.BlockSpec(memory_space=pltpu.VMEM) for _ in range(count)]


def sides(window):
    width = window.shape[1]
    both = pltpu.roll(window, 1, axis=1) + pltpu.roll(window, width - 1, axis=1)
    return both[:, 128 : width - 128]


def sweep(load, coef_ref, put, first, count, shift, off, width):
    above = load(first - 1)[:, 128 : 128 + width]
    here = load(first)
    for r in range(first, first + count):
        below = load(r + 1)
        mid = here[:, 128 : 128 + width]
        lap = (above + below[:, 128 : 128 + width]) + sides(here) - 4.0 * mid
        put(r, mid + coef_ref[r + shift : r + shift + 1, pl.ds(off, width)] * lap)
        above, here = mid, below


def edges_of(index, width, total):
    off = pl.multiple_of(index * width, width)
    before = pl.multiple_of(jnp.maximum(off - 128, 0), 128)
    after = pl.multiple_of(jnp.minimum(off + width, total - 128), 128)
    return off, before, after


def framed(left, mid, right, index, count):
    left = jnp.where(index > 0, left, 0.0)
    right = jnp.where(index < count - 1, right, 0.0)
    return jnp.concatenate([left, mid, right], axis=1)


CHUNK = 512


def ends_kernel(x_ref, field_ref, one_ref, two_ref):
    members, rows, width = x_ref.shape
    odd = is_odd()

    def put(where, low, high):
        one_ref[:, where] = jnp.where(odd, low, high).astype(BF16)
        two_ref[:, where] = jnp.where(odd, high, low).astype(BF16)

    def some(c, carry):
        off = pl.multiple_of(c * CHUNK, CHUNK)
        tall = [x_ref[m, :, pl.ds(off, CHUNK)].astype(F32) for m in range(members)]
        for k in range(2):
            low = jnp.concatenate([t[k : k + 1] for t in tall], axis=0)
            high = jnp.concatenate([t[rows - 2 + k : rows - 1 + k] for t in tall], axis=0)
            put(pl.ds(pl.multiple_of(k * width + off, CHUNK), CHUNK), low, high)
        return carry

    lax.fori_loop(0, width // CHUNK, some, 0)
    piece = width // members

    def folded(row):
        lines = [field_ref[row : row + 1, s * piece : (s + 1) * piece] for s in range(members)]
        whole = jnp.concatenate(lines, axis=0)
        high, rest = halves(whole)
        low = whole - high.astype(F32) - rest.astype(F32)
        return [high.astype(F32), rest.astype(F32), low]

    for k, (low, high) in enumerate(zip(folded(0), folded(1))):
        begin = 2 * width + k * piece
        put(slice(begin, begin + piece), low, high)


def ends(x, field):
    members, _, width = x.shape
    shape = jax.ShapeDtypeStruct((members, 2 * width + 3 * width // members), BF16)
    return pl.pallas_call(
        ends_kernel,
        out_shape=(shape, shape),
        in_specs=vmem_specs(2),
        out_specs=tuple(vmem_specs(2)),
        compiler_params=params(),
        name="ends",
    )(x, field)


def first_pass(source, coef_ref, v1_ref, index, width, spans, shift):
    off, before, after = edges_of(index, CHUNK, width)

    def load(r):
        pieces = [source(r, o, s) for o, s in ((before, 128), (off, CHUNK), (after, 128))]
        return framed(*pieces, index, width // CHUNK)

    for begin, count in spans:

        def put(r, value):
            v1_ref[r + 1, :, pl.ds(off, CHUNK)] = value

        sweep(load, coef_ref, put, begin, count, shift, off, CHUNK)


def second_pass(coef_ref, v1_ref, out_ref, index, width, spans, shift):
    cols = width // out_ref.shape[0]
    each = CHUNK // cols
    off, before, after = edges_of(index, CHUNK, width)

    def load(r):
        pieces = [v1_ref[r + 1, :, pl.ds(o, s)] for o, s in ((before, 128), (off, CHUNK), (after, 128))]
        return framed(*pieces, index, width // CHUNK)

    def put(r, value):
        for k in range(each):
            out_ref[index * each + k, :, r * cols : (r + 1) * cols] = value[
                :, k * cols : (k + 1) * cols
            ].astype(BF16)

    for begin, count in spans:
        sweep(load, coef_ref, put, begin, count, shift, off, CHUNK)


def inner_kernel(x_ref, field_ref, out_ref, v1_ref):
    rows, _, width = x_ref.shape

    def first(c, carry):
        def source(r, off, size):
            return x_ref[r, :, pl.ds(off, size)].astype(F32)

        first_pass(source, field_ref, v1_ref, c, width, ((1, rows - 2),), 0)
        return carry

    def second(c, carry):
        second_pass(field_ref, v1_ref, out_ref, c, width, ((2, rows - 4),), 0)
        return carry

    lax.fori_loop(0, width // CHUNK, first, 0)
    lax.fori_loop(0, width // CHUNK, second, 0)


def inner_forecast(x, field, patches):
    rows, members, width = x.shape
    return pl.pallas_call(
        inner_kernel,
        out_shape=jax.ShapeDtypeStruct((patches, members, rows * width // patches), BF16),
        in_specs=vmem_specs(2),
        out_specs=pl.BlockSpec(memory_space=pltpu.VMEM),
        scratch_shapes=[pltpu.VMEM((rows + 2, members, width), F32)],
        compiler_params=params(),
        name="inner",
    )(x, field)


def outer_kernel(x_ref, one_ref, two_ref, field_ref, part_ref, out_ref, v1_ref, coef_ref):
    rows, members, width = x_ref.shape
    del part_ref
    odd = is_odd()
    piece = width // members
    coef_ref[pl.ds(8, rows), :] = field_ref[...]
    one = one_ref[:, 2 * width :].astype(F32)
    two = two_ref[:, 2 * width :].astype(F32)
    one = one[:, :piece] + one[:, piece : 2 * piece] + one[:, 2 * piece :]
    two = two[:, :piece] + two[:, piece : 2 * piece] + two[:, 2 * piece :]
    low = jnp.where(odd, one, two)
    high = jnp.where(odd, two, one)
    for s in range(members):
        coef_ref[7:8, s * piece : (s + 1) * piece] = low[s : s + 1]
        coef_ref[8 + rows : 9 + rows, s * piece : (s + 1) * piece] = high[s : s + 1]

    def first(c, carry):
        def source(r, off, size):
            if 0 <= r < rows:
                return x_ref[r, :, pl.ds(off, size)].astype(F32)
            at = (r + 2 if r < 0 else r - rows) * width
            a = one_ref[:, pl.ds(at + off, size)].astype(F32)
            b = two_ref[:, pl.ds(at + off, size)].astype(F32)
            return jnp.where(odd, a, b) if r < 0 else jnp.where(odd, b, a)

        first_pass(source, coef_ref, v1_ref, c, width, ((-1, 4), (rows - 3, 4)), 8)
        return carry

    def second(c, carry):
        second_pass(coef_ref, v1_ref, out_ref, c, width, ((0, 2), (rows - 2, 2)), 8)
        return carry

    lax.fori_loop(0, width // CHUNK, first, 0, unroll=2)
    lax.fori_loop(0, width // CHUNK, second, 0, unroll=4)


def outer_forecast(x, one, two, field, part):
    rows, members, width = x.shape
    return pl.pallas_call(
        outer_kernel,
        out_shape=jax.ShapeDtypeStruct(part.shape, BF16),
        in_specs=vmem_specs(5),
        out_specs=pl.BlockSpec(memory_space=pltpu.VMEM),
        scratch_shapes=[pltpu.VMEM((rows + 2, members, width), F32), pltpu.VMEM((rows + 16, width), F32)],
        input_output_aliases={4: 0},
        compiler_params=params(),
        name="outer",
    )(x, one, two, field, part)


def gram_kernel(block_ref, site_ref, value_ref, weight_ref, out_ref):
    groups, each, cells = block_ref.shape
    members = groups * each
    count = site_ref.shape[1]
    half = members // 2
    step = 512
    site = site_ref[...]
    observed = jnp.zeros((members, count), F32)
    for c in range(cells // step):
        cell = lax.broadcasted_iota(jnp.int32, (step, count), 0) + c * step
        chosen = jnp.where(cell == site, 1.0, 0.0).astype(BF16)
        piece = block_ref[:, :, c * step : (c + 1) * step].reshape(members, step)
        observed += jnp.dot(piece, chosen, preferred_element_type=F32)
    mean = jnp.sum(observed, axis=0, keepdims=True) * (1.0 / members)
    root = jnp.sqrt(weight_ref[...])
    spread = ((observed - mean) * root).astype(BF16)
    innovation = ((value_ref[...] - mean) * root).astype(BF16)
    tail = jnp.broadcast_to(innovation.astype(F32), (16, count)).astype(BF16)
    left = jnp.concatenate([spread, tail], axis=0)
    both = lax.dot_general(left, spread, (((1,), (1,)), ((), ())), preferred_element_type=F32)
    low = both[half:members, half:]
    across = lax.broadcasted_iota(jnp.int32, (half, half), 0)
    along = lax.broadcasted_iota(jnp.int32, (half, half), 1)
    corner = jnp.sum(jnp.where(across == along, low, 0.0), axis=0, keepdims=True)
    out_ref[:half, :half] = jnp.where(across <= along, both[:half, :half], low)
    out_ref[:half, half:] = both[:half, half:]
    out_ref[half:, :] = both[members : members + 8]
    out_ref[half + 1 : half + 2, :half] = corner


def gram_of(blocks, sites, values, weights):
    members = blocks.shape[0] * blocks.shape[1]
    return pl.pallas_call(
        gram_kernel,
        out_shape=jax.ShapeDtypeStruct((members // 2 + 8, members), F32),
        in_specs=vmem_specs(4),
        out_specs=pl.BlockSpec(memory_space=pltpu.VMEM),
        compiler_params=params(),
        name="gram",
    )(blocks, sites, values, weights)


def unpacked(packed, half):
    across = lax.broadcasted_iota(jnp.int32, (half, half), 0)
    along = lax.broadcasted_iota(jnp.int32, (half, half), 1)
    block = packed[:half, :half]
    turned = block.T
    upper = jnp.where(across <= along, block, turned)
    lower = jnp.where(across > along, block, turned)
    lower = jnp.where(across == along, packed[half + 1 : half + 2, :half], lower)
    side = packed[:half, half:]
    return jnp.concatenate(
        [jnp.concatenate([upper, side], axis=1), jnp.concatenate([side.T, lower], axis=1)], axis=0
    )


def halves(value):
    high = value.astype(BF16)
    return high, (value - high.astype(F32)).astype(BF16)


def product(left, right):
    lh, ll = left
    rh, rl = right
    return (
        jnp.dot(lh, rh, preferred_element_type=F32)
        + jnp.dot(lh, rl, preferred_element_type=F32)
        + jnp.dot(ll, rh, preferred_element_type=F32)
    )


def root_kernel(one_ref, mid_ref, two_ref, out_ref, root_ref, inverse_ref):
    members = out_ref.shape[0]
    half = members // 2
    packed = mid_ref[...] + 0.5 * (one_ref[...] + two_ref[...])
    vector = packed[half : half + 8]
    gram = unpacked(packed, half)
    across = lax.broadcasted_iota(jnp.int32, (members, members), 0)
    along = lax.broadcasted_iota(jnp.int32, (members, members), 1)
    on_diagonal = across == along
    system = jnp.where(on_diagonal, gram + (members - 1.0), gram)
    squares = jnp.sum(jnp.sum(system * system, axis=0, keepdims=True), axis=1, keepdims=True)
    frob = jnp.sqrt(squares)
    root = system / frob

    def factor_of(value):
        return jnp.where(on_diagonal, 1.5 - 0.5 * value, -0.5 * value)

    def keep(ref, pair):
        ref[0], ref[1] = pair

    def kept(ref):
        return ref[0], ref[1]

    factor_h = halves(factor_of(root))
    keep(inverse_ref, factor_h)
    keep(root_ref, halves(product(halves(root), factor_h)))

    def newton(step, carry):
        factor_h = halves(factor_of(product(kept(inverse_ref), kept(root_ref))))
        new_root = product(kept(root_ref), factor_h)
        new_inverse = product(factor_h, kept(inverse_ref))
        keep(root_ref, halves(new_root))
        keep(inverse_ref, halves(new_inverse))
        return carry

    lax.fori_loop(1, ITERS - 1, newton, 0)
    factor_h = halves(factor_of(product(kept(inverse_ref), kept(root_ref))))
    inverse = product(factor_h, kept(inverse_ref))
    inverse_h = halves(inverse)
    weights = product(halves(product(halves(vector), inverse_h)), inverse_h) / frob
    scale = jnp.sqrt(members - 1.0) * lax.rsqrt(frob)
    out_ref[...] = (scale * inverse + weights[0:1]).astype(BF16)


def root_of(one, mid, two):
    members = mid.shape[1]
    return pl.pallas_call(
        root_kernel,
        out_shape=jax.ShapeDtypeStruct((members, members), BF16),
        in_specs=vmem_specs(3),
        out_specs=pl.BlockSpec(memory_space=pltpu.VMEM),
        scratch_shapes=[pltpu.VMEM((2, members, members), BF16)] * 2,
        compiler_params=params(),
        name="root",
    )(one, mid, two)


def center_kernel(block_ref, mean_ref, out_ref):
    groups, each, cells = block_ref.shape
    members = groups * each
    step = 256

    def one(c, carry):
        where = pl.ds(pl.multiple_of(c * step, step), step)
        cellwise = block_ref[:, :, where].astype(F32)
        mean = jnp.sum(jnp.sum(cellwise, axis=0), axis=0, keepdims=True) * (1.0 / members)
        mean_ref[:, where] = mean
        out_ref[:, where] = (cellwise.reshape(members, step) - mean).astype(BF16)
        return carry

    lax.fori_loop(0, cells // step, one, 0, unroll=2)


def centered(blocks):
    groups, each, cells = blocks.shape
    return pl.pallas_call(
        center_kernel,
        out_shape=(
            jax.ShapeDtypeStruct((1, cells), F32),
            jax.ShapeDtypeStruct((groups * each, cells), BF16),
        ),
        in_specs=vmem_specs(1),
        out_specs=tuple(vmem_specs(2)),
        compiler_params=params(),
        name="center",
    )(blocks)


def update_kernel(turned_ref, mean_ref, deviation_ref, out_ref):
    groups, each, cells = out_ref.shape
    step = 512

    def one(c, carry):
        where = pl.ds(pl.multiple_of(c * step, step), step)
        moved = jnp.dot(turned_ref[...], deviation_ref[:, where], preferred_element_type=F32)
        out_ref[:, :, where] = (mean_ref[:, where] + moved).reshape(groups, each, step).astype(BF16)
        return carry

    lax.fori_loop(0, cells // step, one, 0, unroll=2)


def update(turned, mean, deviation, shape):
    return pl.pallas_call(
        update_kernel,
        out_shape=jax.ShapeDtypeStruct(shape, BF16),
        in_specs=vmem_specs(3),
        out_specs=pl.BlockSpec(memory_space=pltpu.VMEM),
        compiler_params=params(),
        name="update",
    )(turned, mean, deviation)


def edges_kernel(block_ref, one_ref, two_ref):
    cols = one_ref.shape[2]
    odd = is_odd()
    for q in range(block_ref.shape[0]):
        first = block_ref[q, :, :cols].astype(F32)
        last = block_ref[q, :, -cols:].astype(F32)
        one_ref[q] = jnp.where(odd, first, last).astype(BF16)
        two_ref[q] = jnp.where(odd, last, first).astype(BF16)


def edges(blocks, cols):
    shape = jax.ShapeDtypeStruct((*blocks.shape[:2], cols), BF16)
    return pl.pallas_call(
        edges_kernel,
        out_shape=(shape, shape),
        in_specs=vmem_specs(1),
        out_specs=tuple(vmem_specs(2)),
        compiler_params=params(),
        name="edges",
    )(blocks)


def final_rows(source, coef_ref, put, index, cols, patches, spans):
    each = CHUNK // cols
    base = index * each
    off = pl.multiple_of(index * CHUNK, CHUNK)
    before = jnp.maximum(base - 1, 0)
    after = jnp.minimum(base + each, patches - 1)

    def load(r):
        left = source(r, before, cols - 128, cols)
        mid = jnp.concatenate([source(r, base + k, 0, cols) for k in range(each)], axis=1)
        return framed(left, mid, source(r, after, 0, 128), index, patches // each)

    for begin, count in spans:
        sweep(load, coef_ref, put, begin, count, 0, off, CHUNK)


def middle_kernel(block_ref, coef_ref, out_ref, lines_ref):
    patches, members, cells = block_ref.shape
    rows = coef_ref.shape[0]
    cols = cells // rows
    pitch = rows + 8
    lines_ref[...] = jnp.zeros_like(lines_ref)

    def one(c, carry):
        off = pl.multiple_of(c * CHUNK, CHUNK)

        def source(r, q, begin, end):
            return block_ref[q, :, r * cols + begin : r * cols + end].astype(F32)

        def put(r, value):
            for k in range(CHUNK // 128):
                lines_ref[k, pl.ds(r, members, stride=pitch), :] = value[:, k * 128 : (k + 1) * 128]

        final_rows(source, coef_ref, put, c, cols, patches, ((1, rows - 2),))
        for m in range(members):
            tiles = [lines_ref[k, m * pitch : m * pitch + rows, :] for k in range(CHUNK // 128)]
            out_ref[m, :, pl.ds(off, CHUNK)] = jnp.concatenate(tiles, axis=1).astype(BF16)
        return carry

    lax.fori_loop(0, patches * cols // CHUNK, one, 0)


def middle_rows(blocks, coef):
    _, members, _ = blocks.shape
    rows, width = coef.shape
    return pl.pallas_call(
        middle_kernel,
        out_shape=jax.ShapeDtypeStruct((members, rows, width), BF16),
        in_specs=vmem_specs(2),
        out_specs=pl.BlockSpec(memory_space=pltpu.VMEM),
        scratch_shapes=[pltpu.VMEM((CHUNK // 128, members * (rows + 8), 128), F32)],
        compiler_params=params(),
        name="middle",
    )(blocks, coef)


def rim_kernel(block_ref, one_ref, two_ref, coef_ref, part_ref, out_ref, whole_ref, ends_ref, done):
    patches, members, cells = block_ref.shape
    rows = coef_ref.shape[0]
    cols = cells // rows
    chunks = patches * cols // CHUNK
    odd = is_odd()
    line = lax.broadcasted_iota(jnp.int32, (rows, CHUNK), 0)

    def source(r, q, begin, end):
        if 0 <= r < rows:
            return block_ref[q, :, r * cols + begin : r * cols + end].astype(F32)
        a = one_ref[q, :, begin:end].astype(F32)
        b = two_ref[q, :, begin:end].astype(F32)
        return jnp.where(odd, a, b) if r < 0 else jnp.where(odd, b, a)

    def one(c, carry):
        off = pl.multiple_of(c * CHUNK, CHUNK)

        def put(r, value):
            ends_ref[min(r, 1), :, pl.ds(off, CHUNK)] = value

        final_rows(source, coef_ref, put, c, cols, patches, ((0, 1), (rows - 1, 1)))
        return carry

    lax.fori_loop(0, chunks, one, 0, unroll=4)

    def move(c):
        where = pl.ds(pl.multiple_of(c * CHUNK, CHUNK), CHUNK)
        return pltpu.make_async_copy(whole_ref.at[:, :, where], out_ref.at[:, :, where], done.at[c])

    def merge(c, carry):
        where = pl.ds(pl.multiple_of(c * CHUNK, CHUNK), CHUNK)
        for m in range(members):
            old = part_ref[m, :, where].astype(F32)
            new = jnp.where(line == 0, ends_ref[0, m : m + 1, where], old)
            new = jnp.where(line == rows - 1, ends_ref[1, m : m + 1, where], new)
            whole_ref[m, :, where] = new.astype(BF16)
        move(c).start()
        return carry

    lax.fori_loop(0, chunks, merge, 0)

    def settle(c, carry):
        move(c).wait()
        return carry

    lax.fori_loop(0, chunks, settle, 0)


def rim_rows(blocks, one, two, coef, part):
    members, _, width = part.shape
    return pl.pallas_call(
        rim_kernel,
        out_shape=jax.ShapeDtypeStruct(part.shape, BF16),
        in_specs=vmem_specs(5),
        out_specs=pl.BlockSpec(memory_space=pl.ANY),
        scratch_shapes=[
            pltpu.VMEM(part.shape, BF16),
            pltpu.VMEM((2, members, width), F32),
            pltpu.SemaphoreType.DMA((width // CHUNK,)),
        ],
        compiler_params=params(),
        name="rim",
    )(blocks, one, two, coef, part)


def swaps(axis, in_one, in_two):
    count = lax.axis_size(axis)

    def pairs(first):
        both = [(i, i + 1) for i in range(first, count - 1, 2)]
        return both + [(j, i) for i, j in both]

    two = lax.ppermute(in_two, axis, pairs(1))
    one = lax.ppermute(in_one, axis, pairs(0))
    return one, two


def body(
    prior_samples,
    diffusivity_field,
    measured_site_position,
    measured_quantities,
    measurement_weightings,
):
    patches = lax.axis_size(MEM)
    _, rows, width = prior_samples.shape
    cols = width // patches
    one, two = swaps("space", *ends(prior_samples, diffusivity_field[:: rows - 1]))
    turned_prior = jnp.swapaxes(prior_samples, 0, 1)
    part = inner_forecast(turned_prior, diffusivity_field, patches)
    blocks = outer_forecast(turned_prior, one, two, diffusivity_field, part)
    gathered = lax.all_to_all(blocks, MEM, 0, 0, tiled=True)
    own = gram_of(
        gathered, measured_site_position[0], measured_quantities[0], measurement_weightings[0]
    )
    one, two = swaps(MEM, own, own)
    mean, deviation = centered(gathered)
    band = own + 0.5 * (one + two)
    one, two = swaps("space", band, band)
    updated = update(root_of(one, band, two), mean, deviation, gathered.shape)
    returned = lax.all_to_all(updated, MEM, 0, 0, tiled=True)
    one, two = swaps("space", *edges(returned, cols))
    part = middle_rows(returned, diffusivity_field)
    return rim_rows(returned, one, two, diffusivity_field, part)


def solution(mesh):
    finer = Mesh(
        mesh.devices.reshape(2, 8, 2, mesh.shape["space"]), ("mem_0", "mem_1", "mem_2", "space")
    )
    in_specs = (
        P(MEM, "space", None),
        P("space", None),
        P("space", MEM, None),
        P("space", MEM, None),
        P("space", MEM, None),
    )
    out_specs = P(MEM, "space", None)
    return jax.shard_map(body, mesh=finer, in_specs=in_specs, out_specs=out_specs, check_vma=False)
```

```python
import jax
import jax.numpy as jnp
from jax import lax
from jax.experimental import pallas as pl
from jax.experimental.pallas import tpu as pltpu
from jax.sharding import Mesh
from jax.sharding import PartitionSpec as P

ITERS = 10
MEM = ("mem_0", "mem_1", "mem_2")
F32 = jnp.float32
BF16 = jnp.bfloat16
VMEM_LIMIT = 48 << 20


def params():
    return pltpu.CompilerParams(vmem_limit_bytes=VMEM_LIMIT)


def is_odd():
    return lax.bitwise_and(lax.axis_index("space"), 1) > 0


def vmem_specs(count):
    return [pl.BlockSpec(memory_space=pltpu.VMEM) for _ in range(count)]


def sides(window):
    width = window.shape[1]
    both = pltpu.roll(window, 1, axis=1) + pltpu.roll(window, width - 1, axis=1)
    return both[:, 128 : width - 128]


def sweep(load, coef_ref, put, first, count, shift, off, width):
    above = load(first - 1)[:, 128 : 128 + width]
    here = load(first)
    for r in range(first, first + count):
        below = load(r + 1)
        mid = here[:, 128 : 128 + width]
        lap = (above + below[:, 128 : 128 + width]) + sides(here) - 4.0 * mid
        put(r, mid + coef_ref[r + shift : r + shift + 1, pl.ds(off, width)] * lap)
        above, here = mid, below


def edges_of(index, width, total):
    off = pl.multiple_of(index * width, width)
    before = pl.multiple_of(jnp.maximum(off - 128, 0), 128)
    after = pl.multiple_of(jnp.minimum(off + width, total - 128), 128)
    return off, before, after


def framed(left, mid, right, index, count):
    left = jnp.where(index > 0, left, 0.0)
    right = jnp.where(index < count - 1, right, 0.0)
    return jnp.concatenate([left, mid, right], axis=1)


CHUNK = 512


def ends_kernel(x_ref, field_ref, one_ref, two_ref):
    members, rows, width = x_ref.shape
    odd = is_odd()

    def put(where, low, high):
        one_ref[:, where] = jnp.where(odd, low, high).astype(BF16)
        two_ref[:, where] = jnp.where(odd, high, low).astype(BF16)

    def some(c, carry):
        off = pl.multiple_of(c * CHUNK, CHUNK)
        tall = [x_ref[m, :, pl.ds(off, CHUNK)].astype(F32) for m in range(members)]
        for k in range(2):
            low = jnp.concatenate([t[k : k + 1] for t in tall], axis=0)
            high = jnp.concatenate([t[rows - 2 + k : rows - 1 + k] for t in tall], axis=0)
            put(pl.ds(pl.multiple_of(k * width + off, CHUNK), CHUNK), low, high)
        return carry

    lax.fori_loop(0, width // CHUNK, some, 0, unroll=2)
    piece = width // members

    def folded(row):
        lines = [field_ref[row : row + 1, s * piece : (s + 1) * piece] for s in range(members)]
        whole = jnp.concatenate(lines, axis=0)
        high, rest = halves(whole)
        low = whole - high.astype(F32) - rest.astype(F32)
        return [high.astype(F32), rest.astype(F32), low]

    for k, (low, high) in enumerate(zip(folded(0), folded(rows - 1))):
        begin = 2 * width + k * piece
        put(slice(begin, begin + piece), low, high)


def ends(x, field):
    members, _, width = x.shape
    shape = jax.ShapeDtypeStruct((members, 2 * width + 3 * width // members), BF16)
    return pl.pallas_call(
        ends_kernel,
        out_shape=(shape, shape),
        in_specs=vmem_specs(2),
        out_specs=tuple(vmem_specs(2)),
        compiler_params=params(),
        name="ends",
    )(x, field)


def first_pass(source, coef_ref, v1_ref, index, width, spans, shift):
    off, before, after = edges_of(index, CHUNK, width)

    def load(r):
        pieces = [source(r, o, s) for o, s in ((before, 128), (off, CHUNK), (after, 128))]
        return framed(*pieces, index, width // CHUNK)

    for begin, count in spans:

        def put(r, value):
            v1_ref[r + 1, :, pl.ds(off, CHUNK)] = value

        sweep(load, coef_ref, put, begin, count, shift, off, CHUNK)


def second_pass(coef_ref, v1_ref, out_ref, index, width, spans, shift):
    cols = width // out_ref.shape[0]
    each = CHUNK // cols
    off, before, after = edges_of(index, CHUNK, width)

    def load(r):
        pieces = [v1_ref[r + 1, :, pl.ds(o, s)] for o, s in ((before, 128), (off, CHUNK), (after, 128))]
        return framed(*pieces, index, width // CHUNK)

    def put(r, value):
        for k in range(each):
            out_ref[index * each + k, :, r * cols : (r + 1) * cols] = value[
                :, k * cols : (k + 1) * cols
            ].astype(BF16)

    for begin, count in spans:
        sweep(load, coef_ref, put, begin, count, shift, off, CHUNK)


def inner_kernel(x_ref, field_ref, out_ref, v1_ref):
    rows, _, width = x_ref.shape

    def first(c, carry):
        def source(r, off, size):
            return x_ref[r, :, pl.ds(off, size)].astype(F32)

        first_pass(source, field_ref, v1_ref, c, width, ((1, rows - 2),), 0)
        return carry

    def second(c, carry):
        second_pass(field_ref, v1_ref, out_ref, c, width, ((2, rows - 4),), 0)
        return carry

    lax.fori_loop(0, width // CHUNK, first, 0, unroll=4)
    lax.fori_loop(0, width // CHUNK, second, 0, unroll=4)


def inner_forecast(x, field, patches):
    rows, members, width = x.shape
    return pl.pallas_call(
        inner_kernel,
        out_shape=jax.ShapeDtypeStruct((patches, members, rows * width // patches), BF16),
        in_specs=vmem_specs(2),
        out_specs=pl.BlockSpec(memory_space=pltpu.VMEM),
        scratch_shapes=[pltpu.VMEM((rows + 2, members, width), F32)],
        compiler_params=params(),
        name="inner",
    )(x, field)


def outer_kernel(x_ref, one_ref, two_ref, field_ref, part_ref, out_ref, v1_ref, coef_ref):
    rows, members, width = x_ref.shape
    del part_ref
    odd = is_odd()
    piece = width // members
    coef_ref[pl.ds(8, rows), :] = field_ref[...]
    one = one_ref[:, 2 * width :].astype(F32)
    two = two_ref[:, 2 * width :].astype(F32)
    one = one[:, :piece] + one[:, piece : 2 * piece] + one[:, 2 * piece :]
    two = two[:, :piece] + two[:, piece : 2 * piece] + two[:, 2 * piece :]
    low = jnp.where(odd, one, two)
    high = jnp.where(odd, two, one)
    for s in range(members):
        coef_ref[7:8, s * piece : (s + 1) * piece] = low[s : s + 1]
        coef_ref[8 + rows : 9 + rows, s * piece : (s + 1) * piece] = high[s : s + 1]

    def first(c, carry):
        def source(r, off, size):
            if 0 <= r < rows:
                return x_ref[r, :, pl.ds(off, size)].astype(F32)
            at = (r + 2 if r < 0 else r - rows) * width
            a = one_ref[:, pl.ds(at + off, size)].astype(F32)
            b = two_ref[:, pl.ds(at + off, size)].astype(F32)
            return jnp.where(odd, a, b) if r < 0 else jnp.where(odd, b, a)

        first_pass(source, coef_ref, v1_ref, c, width, ((-1, 4), (rows - 3, 4)), 8)
        return carry

    def second(c, carry):
        second_pass(coef_ref, v1_ref, out_ref, c, width, ((0, 2), (rows - 2, 2)), 8)
        return carry

    lax.fori_loop(0, width // CHUNK, first, 0, unroll=4)
    lax.fori_loop(0, width // CHUNK, second, 0, unroll=4)


def outer_forecast(x, one, two, field, part):
    rows, members, width = x.shape
    return pl.pallas_call(
        outer_kernel,
        out_shape=jax.ShapeDtypeStruct(part.shape, BF16),
        in_specs=vmem_specs(5),
        out_specs=pl.BlockSpec(memory_space=pltpu.VMEM),
        scratch_shapes=[pltpu.VMEM((rows + 2, members, width), F32), pltpu.VMEM((rows + 16, width), F32)],
        input_output_aliases={4: 0},
        compiler_params=params(),
        name="outer",
    )(x, one, two, field, part)


def gram_kernel(block_ref, site_ref, value_ref, weight_ref, out_ref):
    groups, each, cells = block_ref.shape
    members = groups * each
    count = site_ref.shape[1]
    half = members // 2
    step = 512
    site = site_ref[...]
    observed = jnp.zeros((members, count), F32)
    for c in range(cells // step):
        cell = lax.broadcasted_iota(jnp.int32, (step, count), 0) + c * step
        chosen = jnp.where(cell == site, 1.0, 0.0).astype(BF16)
        piece = block_ref[:, :, c * step : (c + 1) * step].reshape(members, step)
        observed += jnp.dot(piece, chosen, preferred_element_type=F32)
    mean = jnp.sum(observed, axis=0, keepdims=True) * (1.0 / members)
    root = jnp.sqrt(weight_ref[...])
    spread = ((observed - mean) * root).astype(BF16)
    innovation = ((value_ref[...] - mean) * root).astype(BF16)
    tail = jnp.broadcast_to(innovation.astype(F32), (16, count)).astype(BF16)
    left = jnp.concatenate([spread, tail], axis=0)
    both = lax.dot_general(left, spread, (((1,), (1,)), ((), ())), preferred_element_type=F32)
    low = both[half:members, half:]
    across = lax.broadcasted_iota(jnp.int32, (half, half), 0)
    along = lax.broadcasted_iota(jnp.int32, (half, half), 1)
    corner = jnp.sum(jnp.where(across == along, low, 0.0), axis=0, keepdims=True)
    out_ref[:half, :half] = jnp.where(across <= along, both[:half, :half], low)
    out_ref[:half, half:] = both[:half, half:]
    out_ref[half:, :] = both[members : members + 8]
    out_ref[half + 1 : half + 2, :half] = corner


def gram_of(blocks, sites, values, weights):
    members = blocks.shape[0] * blocks.shape[1]
    return pl.pallas_call(
        gram_kernel,
        out_shape=jax.ShapeDtypeStruct((members // 2 + 8, members), F32),
        in_specs=vmem_specs(4),
        out_specs=pl.BlockSpec(memory_space=pltpu.VMEM),
        compiler_params=params(),
        name="gram",
    )(blocks, sites, values, weights)


def unpacked(packed, half):
    across = lax.broadcasted_iota(jnp.int32, (half, half), 0)
    along = lax.broadcasted_iota(jnp.int32, (half, half), 1)
    block = packed[:half, :half]
    turned = block.T
    upper = jnp.where(across <= along, block, turned)
    lower = jnp.where(across > along, block, turned)
    lower = jnp.where(across == along, packed[half + 1 : half + 2, :half], lower)
    side = packed[:half, half:]
    return jnp.concatenate(
        [jnp.concatenate([upper, side], axis=1), jnp.concatenate([side.T, lower], axis=1)], axis=0
    )


def halves(value):
    high = value.astype(BF16)
    return high, (value - high.astype(F32)).astype(BF16)


def product(left, right):
    lh, ll = left
    rh, rl = right
    return (
        jnp.dot(lh, rh, preferred_element_type=F32)
        + jnp.dot(lh, rl, preferred_element_type=F32)
        + jnp.dot(ll, rh, preferred_element_type=F32)
    )


def root_kernel(one_ref, mid_ref, two_ref, out_ref, root_ref, inverse_ref):
    members = out_ref.shape[0]
    half = members // 2
    packed = mid_ref[...] + 0.5 * (one_ref[...] + two_ref[...])
    vector = packed[half : half + 8]
    gram = unpacked(packed, half)
    across = lax.broadcasted_iota(jnp.int32, (members, members), 0)
    along = lax.broadcasted_iota(jnp.int32, (members, members), 1)
    on_diagonal = across == along
    system = jnp.where(on_diagonal, gram + (members - 1.0), gram)
    squares = jnp.sum(jnp.sum(system * system, axis=0, keepdims=True), axis=1, keepdims=True)
    frob = jnp.sqrt(squares)
    root = system / frob

    def factor_of(value):
        return jnp.where(on_diagonal, 1.5 - 0.5 * value, -0.5 * value)

    def keep(ref, pair):
        ref[0], ref[1] = pair

    def kept(ref):
        return ref[0], ref[1]

    factor_h = halves(factor_of(root))
    keep(inverse_ref, factor_h)
    keep(root_ref, halves(product(halves(root), factor_h)))

    def newton(step, carry):
        factor_h = halves(factor_of(product(kept(inverse_ref), kept(root_ref))))
        new_root = product(kept(root_ref), factor_h)
        new_inverse = product(factor_h, kept(inverse_ref))
        keep(root_ref, halves(new_root))
        keep(inverse_ref, halves(new_inverse))
        return carry

    lax.fori_loop(1, ITERS - 1, newton, 0)
    factor_h = halves(factor_of(product(kept(inverse_ref), kept(root_ref))))
    inverse = product(factor_h, kept(inverse_ref))
    inverse_h = halves(inverse)
    weights = product(halves(product(halves(vector), inverse_h)), inverse_h) / frob
    scale = jnp.sqrt(members - 1.0) * lax.rsqrt(frob)
    out_ref[...] = (scale * inverse + weights[0:1]).astype(BF16)


def root_of(one, mid, two):
    members = mid.shape[1]
    return pl.pallas_call(
        root_kernel,
        out_shape=jax.ShapeDtypeStruct((members, members), BF16),
        in_specs=vmem_specs(3),
        out_specs=pl.BlockSpec(memory_space=pltpu.VMEM),
        scratch_shapes=[pltpu.VMEM((2, members, members), BF16)] * 2,
        compiler_params=params(),
        name="root",
    )(one, mid, two)


def center_kernel(block_ref, mean_ref, out_ref):
    groups, each, cells = block_ref.shape
    members = groups * each
    step = 256

    def one(c, carry):
        where = pl.ds(pl.multiple_of(c * step, step), step)
        cellwise = block_ref[:, :, where].astype(F32)
        mean = jnp.sum(jnp.sum(cellwise, axis=0), axis=0, keepdims=True) * (1.0 / members)
        mean_ref[:, where] = mean
        out_ref[:, where] = (cellwise.reshape(members, step) - mean).astype(BF16)
        return carry

    lax.fori_loop(0, cells // step, one, 0, unroll=2)


def centered(blocks):
    groups, each, cells = blocks.shape
    return pl.pallas_call(
        center_kernel,
        out_shape=(
            jax.ShapeDtypeStruct((1, cells), F32),
            jax.ShapeDtypeStruct((groups * each, cells), BF16),
        ),
        in_specs=vmem_specs(1),
        out_specs=tuple(vmem_specs(2)),
        compiler_params=params(),
        name="center",
    )(blocks)


def update_kernel(turned_ref, mean_ref, deviation_ref, out_ref):
    groups, each, cells = out_ref.shape
    step = 512

    def one(c, carry):
        where = pl.ds(pl.multiple_of(c * step, step), step)
        moved = jnp.dot(turned_ref[...], deviation_ref[:, where], preferred_element_type=F32)
        out_ref[:, :, where] = (mean_ref[:, where] + moved).reshape(groups, each, step).astype(BF16)
        return carry

    lax.fori_loop(0, cells // step, one, 0, unroll=2)


def update(turned, mean, deviation, shape):
    return pl.pallas_call(
        update_kernel,
        out_shape=jax.ShapeDtypeStruct(shape, BF16),
        in_specs=vmem_specs(3),
        out_specs=pl.BlockSpec(memory_space=pltpu.VMEM),
        compiler_params=params(),
        name="update",
    )(turned, mean, deviation)


def edges_kernel(block_ref, one_ref, two_ref):
    cols = one_ref.shape[2]
    odd = is_odd()
    for q in range(block_ref.shape[0]):
        first = block_ref[q, :, :cols].astype(F32)
        last = block_ref[q, :, -cols:].astype(F32)
        one_ref[q] = jnp.where(odd, first, last).astype(BF16)
        two_ref[q] = jnp.where(odd, last, first).astype(BF16)


def edges(blocks, cols):
    shape = jax.ShapeDtypeStruct((*blocks.shape[:2], cols), BF16)
    return pl.pallas_call(
        edges_kernel,
        out_shape=(shape, shape),
        in_specs=vmem_specs(1),
        out_specs=tuple(vmem_specs(2)),
        compiler_params=params(),
        name="edges",
    )(blocks)


def final_rows(source, coef_ref, put, index, cols, patches, spans):
    each = CHUNK // cols
    base = index * each
    off = pl.multiple_of(index * CHUNK, CHUNK)
    before = jnp.maximum(base - 1, 0)
    after = jnp.minimum(base + each, patches - 1)

    def load(r):
        left = source(r, before, cols - 128, cols)
        mid = jnp.concatenate([source(r, base + k, 0, cols) for k in range(each)], axis=1)
        return framed(left, mid, source(r, after, 0, 128), index, patches // each)

    for begin, count in spans:
        sweep(load, coef_ref, put, begin, count, 0, off, CHUNK)


def middle_kernel(block_ref, coef_ref, out_ref, lines_ref):
    patches, members, cells = block_ref.shape
    rows = coef_ref.shape[0]
    cols = cells // rows
    pitch = rows + 8
    lines_ref[...] = jnp.zeros_like(lines_ref)

    def one(c, carry):
        off = pl.multiple_of(c * CHUNK, CHUNK)

        def source(r, q, begin, end):
            return block_ref[q, :, r * cols + begin : r * cols + end].astype(F32)

        def put(r, value):
            for k in range(CHUNK // 128):
                lines_ref[k, pl.ds(r, members, stride=pitch), :] = value[:, k * 128 : (k + 1) * 128]

        final_rows(source, coef_ref, put, c, cols, patches, ((1, rows - 2),))
        for m in range(members):
            tiles = [lines_ref[k, m * pitch : m * pitch + rows, :] for k in range(CHUNK // 128)]
            out_ref[m, :, pl.ds(off, CHUNK)] = jnp.concatenate(tiles, axis=1).astype(BF16)
        return carry

    lax.fori_loop(0, patches * cols // CHUNK, one, 0, unroll=2)


def middle_rows(blocks, coef):
    _, members, _ = blocks.shape
    rows, width = coef.shape
    return pl.pallas_call(
        middle_kernel,
        out_shape=jax.ShapeDtypeStruct((members, rows, width), BF16),
        in_specs=vmem_specs(2),
        out_specs=pl.BlockSpec(memory_space=pltpu.VMEM),
        scratch_shapes=[pltpu.VMEM((CHUNK // 128, members * (rows + 8), 128), F32)],
        compiler_params=params(),
        name="middle",
    )(blocks, coef)


def rim_kernel(block_ref, one_ref, two_ref, coef_ref, part_ref, out_ref, whole_ref, ends_ref, done):
    patches, members, cells = block_ref.shape
    rows = coef_ref.shape[0]
    cols = cells // rows
    chunks = patches * cols // CHUNK
    odd = is_odd()
    line = lax.broadcasted_iota(jnp.int32, (rows, CHUNK), 0)

    def source(r, q, begin, end):
        if 0 <= r < rows:
            return block_ref[q, :, r * cols + begin : r * cols + end].astype(F32)
        a = one_ref[q, :, begin:end].astype(F32)
        b = two_ref[q, :, begin:end].astype(F32)
        return jnp.where(odd, a, b) if r < 0 else jnp.where(odd, b, a)

    def move(c):
        where = pl.ds(pl.multiple_of(c * CHUNK, CHUNK), CHUNK)
        return pltpu.make_async_copy(whole_ref.at[:, :, where], out_ref.at[:, :, where], done.at[c])

    def one(c, carry):
        where = pl.ds(pl.multiple_of(c * CHUNK, CHUNK), CHUNK)

        def put(r, value):
            ends_ref[min(r, 1), :, where] = value

        final_rows(source, coef_ref, put, c, cols, patches, ((0, 1), (rows - 1, 1)))
        for m in range(members):
            old = part_ref[m, :, where].astype(F32)
            new = jnp.where(line == 0, ends_ref[0, m : m + 1, where], old)
            new = jnp.where(line == rows - 1, ends_ref[1, m : m + 1, where], new)
            whole_ref[m, :, where] = new.astype(BF16)
        move(c).start()
        return carry

    lax.fori_loop(0, chunks, one, 0, unroll=4)

    def settle(c, carry):
        move(c).wait()
        return carry

    lax.fori_loop(0, chunks, settle, 0)


def rim_rows(blocks, one, two, coef, part):
    members, _, width = part.shape
    return pl.pallas_call(
        rim_kernel,
        out_shape=jax.ShapeDtypeStruct(part.shape, BF16),
        in_specs=vmem_specs(5),
        out_specs=pl.BlockSpec(memory_space=pl.ANY),
        scratch_shapes=[
            pltpu.VMEM(part.shape, BF16),
            pltpu.VMEM((2, members, width), F32),
            pltpu.SemaphoreType.DMA((width // CHUNK,)),
        ],
        compiler_params=params(),
        name="rim",
    )(blocks, one, two, coef, part)


def swaps(axis, in_one, in_two):
    count = lax.axis_size(axis)

    def pairs(first):
        both = [(i, i + 1) for i in range(first, count - 1, 2)]
        return both + [(j, i) for i, j in both]

    two = lax.ppermute(in_two, axis, pairs(1))
    one = lax.ppermute(in_one, axis, pairs(0))
    return one, two


def body(
    prior_samples,
    diffusivity_field,
    measured_site_position,
    measured_quantities,
    measurement_weightings,
):
    patches = lax.axis_size(MEM)
    cols = prior_samples.shape[2] // patches
    field = diffusivity_field
    one, two = swaps("space", *ends(prior_samples, field))
    turned_prior = jnp.swapaxes(prior_samples, 0, 1)
    part = inner_forecast(turned_prior, field, patches)
    blocks = outer_forecast(turned_prior, one, two, field, part)
    gathered = lax.all_to_all(blocks, MEM, 0, 0, tiled=True)
    own = gram_of(
        gathered, measured_site_position[0], measured_quantities[0], measurement_weightings[0]
    )
    one, two = swaps(MEM, own, own)
    mean, deviation = centered(gathered)
    band = own + 0.5 * (one + two)
    one, two = swaps("space", band, band)
    updated = update(root_of(one, band, two), mean, deviation, gathered.shape)
    returned = lax.all_to_all(updated, MEM, 0, 0, tiled=True)
    one, two = swaps("space", *edges(returned, cols))
    part = middle_rows(returned, field)
    return rim_rows(returned, one, two, field, part)


def solution(mesh):
    finer = Mesh(
        mesh.devices.reshape(2, 8, 2, mesh.shape["space"]), ("mem_0", "mem_1", "mem_2", "space")
    )
    in_specs = (
        P(MEM, "space", None),
        P("space", None),
        P("space", MEM, None),
        P("space", MEM, None),
        P("space", MEM, None),
    )
    out_specs = P(MEM, "space", None)
    return jax.shard_map(body, mesh=finer, in_specs=in_specs, out_specs=out_specs, check_vma=False)
```

```python
import jax
import jax.numpy as jnp
from jax import lax
from jax.experimental import pallas as pl
from jax.experimental.pallas import tpu as pltpu
from jax.sharding import Mesh
from jax.sharding import PartitionSpec as P

ITERS = 10
MEM = ("mem_0", "mem_1", "mem_2")
F32 = jnp.float32
BF16 = jnp.bfloat16
VMEM_LIMIT = 24 << 20


def params():
    return pltpu.CompilerParams(vmem_limit_bytes=VMEM_LIMIT)


def is_odd():
    return lax.bitwise_and(lax.axis_index("space"), 1) > 0


def vmem_specs(count):
    return [pl.BlockSpec(memory_space=pltpu.VMEM) for _ in range(count)]


def sides(window):
    width = window.shape[1]
    both = pltpu.roll(window, 1, axis=1) + pltpu.roll(window, width - 1, axis=1)
    return both[:, 128 : width - 128]


def sweep(load, coef_ref, put, first, count, shift, off, width):
    above = load(first - 1)[:, 128 : 128 + width]
    here = load(first)
    for r in range(first, first + count):
        below = load(r + 1)
        mid = here[:, 128 : 128 + width]
        lap = (above + below[:, 128 : 128 + width]) + sides(here) - 4.0 * mid
        put(r, mid + coef_ref[r + shift : r + shift + 1, pl.ds(off, width)] * lap)
        above, here = mid, below


def edges_of(index, width, total):
    off = pl.multiple_of(index * width, width)
    before = pl.multiple_of(jnp.maximum(off - 128, 0), 128)
    after = pl.multiple_of(jnp.minimum(off + width, total - 128), 128)
    return off, before, after


def framed(left, mid, right, index, count):
    left = jnp.where(index > 0, left, 0.0)
    right = jnp.where(index < count - 1, right, 0.0)
    return jnp.concatenate([left, mid, right], axis=1)


CHUNK = 512


def ends_kernel(x_hbm, field_hbm, one_ref, two_ref, x_ref, field_ref, arrived):
    members, rows, width = x_ref.shape
    odd = is_odd()
    parts = arrived.shape[0] - 1
    size = width // parts

    def fetch(k):
        where = slice(k * size, (k + 1) * size)
        return pltpu.make_async_copy(x_hbm.at[:, :, where], x_ref.at[:, :, where], arrived.at[k])

    whole = pltpu.make_async_copy(field_hbm, field_ref, arrived.at[parts])
    whole.start()
    for k in range(parts):
        fetch(k).start()

    def put(where, low, high):
        one_ref[:, where] = jnp.where(odd, low, high).astype(BF16)
        two_ref[:, where] = jnp.where(odd, high, low).astype(BF16)

    piece = width // members

    def folded(row):
        lines = [field_ref[row : row + 1, s * piece : (s + 1) * piece] for s in range(members)]
        block = jnp.concatenate(lines, axis=0)
        high, rest = halves(block)
        low = block - high.astype(F32) - rest.astype(F32)
        return [high.astype(F32), rest.astype(F32), low]

    whole.wait()
    for k, (low, high) in enumerate(zip(folded(0), folded(rows - 1))):
        begin = 2 * width + k * piece
        put(slice(begin, begin + piece), low, high)

    def some(c, carry):
        off = pl.multiple_of(c * CHUNK, CHUNK)
        tall = [x_ref[m, :, pl.ds(off, CHUNK)].astype(F32) for m in range(members)]
        for k in range(2):
            low = jnp.concatenate([t[k : k + 1] for t in tall], axis=0)
            high = jnp.concatenate([t[rows - 2 + k : rows - 1 + k] for t in tall], axis=0)
            put(pl.ds(pl.multiple_of(k * width + off, CHUNK), CHUNK), low, high)
        return carry

    each = size // CHUNK
    for k in range(parts):
        fetch(k).wait()
        lax.fori_loop(k * each, (k + 1) * each, some, 0, unroll=2)


def ends(x, field):
    members, _, width = x.shape
    shape = jax.ShapeDtypeStruct((members, 2 * width + 3 * width // members), BF16)
    return pl.pallas_call(
        ends_kernel,
        out_shape=(
            shape,
            shape,
            jax.ShapeDtypeStruct(x.shape, x.dtype),
            jax.ShapeDtypeStruct(field.shape, field.dtype),
        ),
        in_specs=[pl.BlockSpec(memory_space=pltpu.HBM)] * 2,
        out_specs=tuple(vmem_specs(4)),
        scratch_shapes=[pltpu.SemaphoreType.DMA((5,))],
        compiler_params=params(),
        name="ends",
    )(*(pltpu.with_memory_space_constraint(v, pltpu.HBM) for v in (x, field)))


def first_pass(source, coef_ref, keep, index, width, spans, shift):
    off, before, after = edges_of(index, CHUNK, width)

    def load(r):
        pieces = [source(r, o, s) for o, s in ((before, 128), (off, CHUNK), (after, 128))]
        return framed(*pieces, index, width // CHUNK)

    for begin, count in spans:

        def put(r, value):
            keep(r, pl.ds(off, CHUNK), value)

        sweep(load, coef_ref, put, begin, count, shift, off, CHUNK)


def second_pass(coef_ref, pick, out_ref, index, width, spans, shift):
    cols = width // out_ref.shape[0]
    each = CHUNK // cols
    off, before, after = edges_of(index, CHUNK, width)

    def load(r):
        pieces = [pick(r, o, s) for o, s in ((before, 128), (off, CHUNK), (after, 128))]
        return framed(*pieces, index, width // CHUNK)

    def put(r, value):
        for k in range(each):
            out_ref[index * each + k, :, r * cols : (r + 1) * cols] = value[
                :, k * cols : (k + 1) * cols
            ].astype(BF16)

    for begin, count in spans:
        sweep(load, coef_ref, put, begin, count, shift, off, CHUNK)


def inner_kernel(x_ref, field_ref, out_ref, kept_ref, v1_ref):
    rows, _, width = x_ref.shape
    chunks = width // CHUNK
    kept = (1, 2, rows - 3, rows - 2)

    def first(c, carry):
        def source(r, off, size):
            return x_ref[r, :, pl.ds(off, size)].astype(F32)

        def keep(r, where, value):
            v1_ref[r + 1, :, where] = value
            if r in kept:
                kept_ref[kept.index(r), :, where] = value

        first_pass(source, field_ref, keep, c, width, ((1, rows - 2),), 0)
        return carry

    def pick(r, off, size):
        return v1_ref[r + 1, :, pl.ds(off, size)]

    def second(c, carry):
        second_pass(field_ref, pick, out_ref, c, width, ((2, rows - 4),), 0)
        return carry

    lax.fori_loop(0, chunks, first, 0, unroll=4)
    lax.fori_loop(0, chunks, second, 0, unroll=4)


def inner_forecast(x, field, patches):
    rows, members, width = x.shape
    return pl.pallas_call(
        inner_kernel,
        out_shape=(
            jax.ShapeDtypeStruct((patches, members, rows * width // patches), BF16),
            jax.ShapeDtypeStruct((4, members, width), F32),
        ),
        in_specs=vmem_specs(2),
        out_specs=tuple(vmem_specs(2)),
        scratch_shapes=[pltpu.VMEM((rows + 2, members, width), F32)],
        compiler_params=params(),
        name="inner",
    )(x, field)


def outer_kernel(x_ref, one_ref, two_ref, field_ref, part_ref, kept_ref, out_ref, v1_ref, coef_ref):
    rows, members, width = x_ref.shape
    del part_ref
    odd = is_odd()
    piece = width // members
    coef_ref[pl.ds(8, rows), :] = field_ref[...]
    one = one_ref[:, 2 * width :].astype(F32)
    two = two_ref[:, 2 * width :].astype(F32)
    one = one[:, :piece] + one[:, piece : 2 * piece] + one[:, 2 * piece :]
    two = two[:, :piece] + two[:, piece : 2 * piece] + two[:, 2 * piece :]
    low = jnp.where(odd, one, two)
    high = jnp.where(odd, two, one)
    for s in range(members):
        coef_ref[7:8, s * piece : (s + 1) * piece] = low[s : s + 1]
        coef_ref[8 + rows : 9 + rows, s * piece : (s + 1) * piece] = high[s : s + 1]

    def first(c, carry):
        def source(r, off, size):
            if 0 <= r < rows:
                return x_ref[r, :, pl.ds(off, size)].astype(F32)
            at = (r + 2 if r < 0 else r - rows) * width
            a = one_ref[:, pl.ds(at + off, size)].astype(F32)
            b = two_ref[:, pl.ds(at + off, size)].astype(F32)
            return jnp.where(odd, a, b) if r < 0 else jnp.where(odd, b, a)

        def keep(r, where, value):
            v1_ref[r + 1, :, where] = value

        first_pass(source, coef_ref, keep, c, width, ((-1, 2), (rows - 1, 2)), 8)
        return carry

    kept = (1, 2, rows - 3, rows - 2)

    def pick(r, off, size):
        if r in kept:
            return kept_ref[kept.index(r), :, pl.ds(off, size)]
        return v1_ref[r + 1, :, pl.ds(off, size)]

    def second(c, carry):
        second_pass(coef_ref, pick, out_ref, c, width, ((0, 2), (rows - 2, 2)), 8)
        return carry

    lax.fori_loop(0, width // CHUNK, first, 0, unroll=4)
    lax.fori_loop(0, width // CHUNK, second, 0, unroll=4)


def outer_forecast(x, one, two, field, part, kept):
    rows, members, width = x.shape
    return pl.pallas_call(
        outer_kernel,
        out_shape=jax.ShapeDtypeStruct(part.shape, BF16),
        in_specs=vmem_specs(6),
        out_specs=pl.BlockSpec(memory_space=pltpu.VMEM),
        scratch_shapes=[pltpu.VMEM((rows + 2, members, width), F32), pltpu.VMEM((rows + 16, width), F32)],
        input_output_aliases={4: 0},
        compiler_params=params(),
        name="outer",
    )(x, one, two, field, part, kept)


def gram_kernel(block_ref, site_ref, value_ref, weight_ref, out_ref):
    groups, each, cells = block_ref.shape
    members = groups * each
    count = site_ref.shape[1]
    half = members // 2
    step = 512
    site = site_ref[...]
    observed = jnp.zeros((members, count), F32)
    for c in range(cells // step):
        cell = lax.broadcasted_iota(jnp.int32, (step, count), 0) + c * step
        chosen = jnp.where(cell == site, 1.0, 0.0).astype(BF16)
        piece = block_ref[:, :, c * step : (c + 1) * step].reshape(members, step)
        observed += jnp.dot(piece, chosen, preferred_element_type=F32)
    mean = jnp.sum(observed, axis=0, keepdims=True) * (1.0 / members)
    root = jnp.sqrt(weight_ref[...])
    spread = ((observed - mean) * root).astype(BF16)
    innovation = ((value_ref[...] - mean) * root).astype(BF16)
    tail = jnp.broadcast_to(innovation.astype(F32), (16, count)).astype(BF16)
    left = jnp.concatenate([spread, tail], axis=0)
    both = lax.dot_general(left, spread, (((1,), (1,)), ((), ())), preferred_element_type=F32)
    low = both[half:members, half:]
    across = lax.broadcasted_iota(jnp.int32, (half, half), 0)
    along = lax.broadcasted_iota(jnp.int32, (half, half), 1)
    corner = jnp.sum(jnp.where(across == along, low, 0.0), axis=0, keepdims=True)
    out_ref[:half, :half] = jnp.where(across <= along, both[:half, :half], low)
    out_ref[:half, half:] = both[:half, half:]
    out_ref[half:, :] = both[members : members + 8]
    out_ref[half + 1 : half + 2, :half] = corner


def gram_of(blocks, sites, values, weights):
    members = blocks.shape[0] * blocks.shape[1]
    return pl.pallas_call(
        gram_kernel,
        out_shape=jax.ShapeDtypeStruct((members // 2 + 8, members), F32),
        in_specs=vmem_specs(4),
        out_specs=pl.BlockSpec(memory_space=pltpu.VMEM),
        compiler_params=params(),
        name="gram",
    )(blocks, sites, values, weights)


def unpacked(packed, half):
    across = lax.broadcasted_iota(jnp.int32, (half, half), 0)
    along = lax.broadcasted_iota(jnp.int32, (half, half), 1)
    block = packed[:half, :half]
    turned = block.T
    upper = jnp.where(across <= along, block, turned)
    lower = jnp.where(across > along, block, turned)
    lower = jnp.where(across == along, packed[half + 1 : half + 2, :half], lower)
    side = packed[:half, half:]
    return jnp.concatenate(
        [jnp.concatenate([upper, side], axis=1), jnp.concatenate([side.T, lower], axis=1)], axis=0
    )


def halves(value):
    high = value.astype(BF16)
    return high, (value - high.astype(F32)).astype(BF16)


def product(left, right):
    lh, ll = left
    rh, rl = right
    return (
        jnp.dot(lh, rh, preferred_element_type=F32)
        + jnp.dot(lh, rl, preferred_element_type=F32)
        + jnp.dot(ll, rh, preferred_element_type=F32)
    )


def root_kernel(one_ref, mid_ref, two_ref, out_ref, root_ref, inverse_ref):
    members = out_ref.shape[0]
    half = members // 2
    packed = mid_ref[...] + 0.5 * (one_ref[...] + two_ref[...])
    vector = packed[half : half + 8]
    gram = unpacked(packed, half)
    across = lax.broadcasted_iota(jnp.int32, (members, members), 0)
    along = lax.broadcasted_iota(jnp.int32, (members, members), 1)
    on_diagonal = across == along
    system = jnp.where(on_diagonal, gram + (members - 1.0), gram)
    squares = jnp.sum(jnp.sum(system * system, axis=0, keepdims=True), axis=1, keepdims=True)
    frob = jnp.sqrt(squares)
    root = system / frob

    def factor_of(value):
        return jnp.where(on_diagonal, 1.5 - 0.5 * value, -0.5 * value)

    def keep(ref, pair):
        ref[0], ref[1] = pair

    def kept(ref):
        return ref[0], ref[1]

    factor_h = halves(factor_of(root))
    keep(inverse_ref, factor_h)
    keep(root_ref, halves(product(halves(root), factor_h)))

    def newton(step, carry):
        factor_h = halves(factor_of(product(kept(inverse_ref), kept(root_ref))))
        new_root = product(kept(root_ref), factor_h)
        new_inverse = product(factor_h, kept(inverse_ref))
        keep(root_ref, halves(new_root))
        keep(inverse_ref, halves(new_inverse))
        return carry

    lax.fori_loop(1, ITERS - 1, newton, 0)
    factor_h = halves(factor_of(product(kept(inverse_ref), kept(root_ref))))
    inverse = product(factor_h, kept(inverse_ref))
    inverse_h = halves(inverse)
    weights = product(halves(product(halves(vector), inverse_h)), inverse_h) / frob
    scale = jnp.sqrt(members - 1.0) * lax.rsqrt(frob)
    out_ref[...] = (scale * inverse + weights[0:1]).astype(BF16)


def root_of(one, mid, two):
    members = mid.shape[1]
    return pl.pallas_call(
        root_kernel,
        out_shape=jax.ShapeDtypeStruct((members, members), BF16),
        in_specs=vmem_specs(3),
        out_specs=pl.BlockSpec(memory_space=pltpu.VMEM),
        scratch_shapes=[pltpu.VMEM((2, members, members), BF16)] * 2,
        compiler_params=params(),
        name="root",
    )(one, mid, two)


def center_kernel(block_ref, mean_ref, out_ref):
    groups, each, cells = block_ref.shape
    members = groups * each
    step = 256

    def one(c, carry):
        where = pl.ds(pl.multiple_of(c * step, step), step)
        cellwise = block_ref[:, :, where].astype(F32)
        mean = jnp.sum(jnp.sum(cellwise, axis=0), axis=0, keepdims=True) * (1.0 / members)
        mean_ref[:, where] = mean
        out_ref[:, where] = (cellwise.reshape(members, step) - mean).astype(BF16)
        return carry

    lax.fori_loop(0, cells // step, one, 0, unroll=2)


def centered(blocks):
    groups, each, cells = blocks.shape
    return pl.pallas_call(
        center_kernel,
        out_shape=(
            jax.ShapeDtypeStruct((1, cells), F32),
            jax.ShapeDtypeStruct((groups * each, cells), BF16),
        ),
        in_specs=vmem_specs(1),
        out_specs=tuple(vmem_specs(2)),
        compiler_params=params(),
        name="center",
    )(blocks)


def update_kernel(turned_ref, mean_ref, deviation_ref, out_ref):
    groups, each, cells = out_ref.shape
    step = 512

    def one(c, carry):
        where = pl.ds(pl.multiple_of(c * step, step), step)
        moved = jnp.dot(turned_ref[...], deviation_ref[:, where], preferred_element_type=F32)
        out_ref[:, :, where] = (mean_ref[:, where] + moved).reshape(groups, each, step).astype(BF16)
        return carry

    lax.fori_loop(0, cells // step, one, 0, unroll=2)


def update(turned, mean, deviation, shape):
    return pl.pallas_call(
        update_kernel,
        out_shape=jax.ShapeDtypeStruct(shape, BF16),
        in_specs=vmem_specs(3),
        out_specs=pl.BlockSpec(memory_space=pltpu.VMEM),
        compiler_params=params(),
        name="update",
    )(turned, mean, deviation)


def edges_kernel(block_ref, one_ref, two_ref):
    cols = one_ref.shape[2]
    odd = is_odd()
    for q in range(block_ref.shape[0]):
        first = block_ref[q, :, :cols].astype(F32)
        last = block_ref[q, :, -cols:].astype(F32)
        one_ref[q] = jnp.where(odd, first, last).astype(BF16)
        two_ref[q] = jnp.where(odd, last, first).astype(BF16)


def edges(blocks, cols):
    shape = jax.ShapeDtypeStruct((*blocks.shape[:2], cols), BF16)
    return pl.pallas_call(
        edges_kernel,
        out_shape=(shape, shape),
        in_specs=vmem_specs(1),
        out_specs=tuple(vmem_specs(2)),
        compiler_params=params(),
        name="edges",
    )(blocks)


def final_rows(source, coef_ref, put, index, cols, patches, spans):
    each = CHUNK // cols
    base = index * each
    off = pl.multiple_of(index * CHUNK, CHUNK)
    before = jnp.maximum(base - 1, 0)
    after = jnp.minimum(base + each, patches - 1)

    def load(r):
        left = source(r, before, cols - 128, cols)
        mid = jnp.concatenate([source(r, base + k, 0, cols) for k in range(each)], axis=1)
        return framed(left, mid, source(r, after, 0, 128), index, patches // each)

    for begin, count in spans:
        sweep(load, coef_ref, put, begin, count, 0, off, CHUNK)


def middle_kernel(block_ref, coef_ref, out_ref, lines_ref):
    patches, members, cells = block_ref.shape
    rows = coef_ref.shape[0]
    cols = cells // rows
    pitch = rows + 8
    lines_ref[...] = jnp.zeros_like(lines_ref)

    def one(c, carry):
        off = pl.multiple_of(c * CHUNK, CHUNK)

        def source(r, q, begin, end):
            return block_ref[q, :, r * cols + begin : r * cols + end].astype(F32)

        def put(r, value):
            for k in range(CHUNK // 128):
                lines_ref[k, pl.ds(r, members, stride=pitch), :] = value[:, k * 128 : (k + 1) * 128]

        final_rows(source, coef_ref, put, c, cols, patches, ((1, rows - 2),))
        for m in range(members):
            tiles = [lines_ref[k, m * pitch : m * pitch + rows, :] for k in range(CHUNK // 128)]
            out_ref[m, :, pl.ds(off, CHUNK)] = jnp.concatenate(tiles, axis=1).astype(BF16)
        return carry

    lax.fori_loop(0, patches * cols // CHUNK, one, 0, unroll=2)


def middle_rows(blocks, coef):
    _, members, _ = blocks.shape
    rows, width = coef.shape
    return pl.pallas_call(
        middle_kernel,
        out_shape=jax.ShapeDtypeStruct((members, rows, width), BF16),
        in_specs=vmem_specs(2),
        out_specs=pl.BlockSpec(memory_space=pltpu.VMEM),
        scratch_shapes=[pltpu.VMEM((CHUNK // 128, members * (rows + 8), 128), F32)],
        compiler_params=params(),
        name="middle",
    )(blocks, coef)


def rim_kernel(block_ref, one_ref, two_ref, coef_ref, part_ref, out_ref, whole_ref, ends_ref, done):
    patches, members, cells = block_ref.shape
    rows = coef_ref.shape[0]
    cols = cells // rows
    chunks = patches * cols // CHUNK
    odd = is_odd()
    line = lax.broadcasted_iota(jnp.int32, (rows, CHUNK), 0)

    def source(r, q, begin, end):
        if 0 <= r < rows:
            return block_ref[q, :, r * cols + begin : r * cols + end].astype(F32)
        a = one_ref[q, :, begin:end].astype(F32)
        b = two_ref[q, :, begin:end].astype(F32)
        return jnp.where(odd, a, b) if r < 0 else jnp.where(odd, b, a)

    def move(c):
        where = pl.ds(pl.multiple_of(c * CHUNK, CHUNK), CHUNK)
        return pltpu.make_async_copy(whole_ref.at[:, :, where], out_ref.at[:, :, where], done.at[c])

    def one(c, carry):
        where = pl.ds(pl.multiple_of(c * CHUNK, CHUNK), CHUNK)

        def put(r, value):
            ends_ref[min(r, 1), :, where] = value

        final_rows(source, coef_ref, put, c, cols, patches, ((0, 1), (rows - 1, 1)))
        for m in range(members):
            old = part_ref[m, :, where].astype(F32)
            new = jnp.where(line == 0, ends_ref[0, m : m + 1, where], old)
            new = jnp.where(line == rows - 1, ends_ref[1, m : m + 1, where], new)
            whole_ref[m, :, where] = new.astype(BF16)
        move(c).start()
        return carry

    lax.fori_loop(0, chunks, one, 0, unroll=4)

    def settle(c, carry):
        move(c).wait()
        return carry

    lax.fori_loop(0, chunks, settle, 0)


def rim_rows(blocks, one, two, coef, part):
    members, _, width = part.shape
    return pl.pallas_call(
        rim_kernel,
        out_shape=jax.ShapeDtypeStruct(part.shape, BF16),
        in_specs=vmem_specs(5),
        out_specs=pl.BlockSpec(memory_space=pl.ANY),
        scratch_shapes=[
            pltpu.VMEM(part.shape, BF16),
            pltpu.VMEM((2, members, width), F32),
            pltpu.SemaphoreType.DMA((width // CHUNK,)),
        ],
        compiler_params=params(),
        name="rim",
    )(blocks, one, two, coef, part)


def swaps(axis, in_one, in_two):
    count = lax.axis_size(axis)

    def pairs(first):
        both = [(i, i + 1) for i in range(first, count - 1, 2)]
        return both + [(j, i) for i, j in both]

    two = lax.ppermute(in_two, axis, pairs(1))
    one = lax.ppermute(in_one, axis, pairs(0))
    return one, two


def body(
    prior_samples,
    diffusivity_field,
    measured_site_position,
    measured_quantities,
    measurement_weightings,
):
    patches = lax.axis_size(MEM)
    cols = prior_samples.shape[2] // patches
    one, two, prior, field = ends(prior_samples, diffusivity_field)
    one, two = swaps("space", one, two)
    turned_prior = jnp.swapaxes(prior, 0, 1)
    part, kept = inner_forecast(turned_prior, field, patches)
    blocks = outer_forecast(turned_prior, one, two, field, part, kept)
    gathered = lax.all_to_all(blocks, MEM, 0, 0, tiled=True)
    own = gram_of(
        gathered, measured_site_position[0], measured_quantities[0], measurement_weightings[0]
    )
    one, two = swaps(MEM, own, own)
    mean, deviation = centered(gathered)
    band = own + 0.5 * (one + two)
    one, two = swaps("space", band, band)
    updated = update(root_of(one, band, two), mean, deviation, gathered.shape)
    returned = lax.all_to_all(updated, MEM, 0, 0, tiled=True)
    one, two = swaps("space", *edges(returned, cols))
    part = middle_rows(returned, field)
    return rim_rows(returned, one, two, field, part)


def solution(mesh):
    finer = Mesh(
        mesh.devices.reshape(2, 8, 2, mesh.shape["space"]), ("mem_0", "mem_1", "mem_2", "space")
    )
    in_specs = (
        P(MEM, "space", None),
        P("space", None),
        P("space", MEM, None),
        P("space", MEM, None),
        P("space", MEM, None),
    )
    out_specs = P(MEM, "space", None)
    return jax.shard_map(body, mesh=finer, in_specs=in_specs, out_specs=out_specs, check_vma=False)
```

```python
import jax
import jax.numpy as jnp
from jax import lax
from jax.experimental import pallas as pl
from jax.experimental.pallas import tpu as pltpu
from jax.sharding import Mesh
from jax.sharding import PartitionSpec as P

ITERS = 10
MEM = ("mem_0", "mem_1", "mem_2")
F32 = jnp.float32
BF16 = jnp.bfloat16
VMEM_LIMIT = 24 << 20


def params():
    return pltpu.CompilerParams(vmem_limit_bytes=VMEM_LIMIT)


def is_odd():
    return lax.bitwise_and(lax.axis_index("space"), 1) > 0


def vmem_specs(count):
    return [pl.BlockSpec(memory_space=pltpu.VMEM) for _ in range(count)]


def sides(window):
    width = window.shape[1]
    both = pltpu.roll(window, 1, axis=1) + pltpu.roll(window, width - 1, axis=1)
    return both[:, 128 : width - 128]


def sweep(load, coef_ref, put, first, count, shift, off, width):
    above = load(first - 1)[:, 128 : 128 + width]
    here = load(first)
    for r in range(first, first + count):
        below = load(r + 1)
        mid = here[:, 128 : 128 + width]
        lap = (above + below[:, 128 : 128 + width]) + sides(here) - 4.0 * mid
        put(r, mid + coef_ref[r + shift : r + shift + 1, pl.ds(off, width)] * lap)
        above, here = mid, below


def edges_of(index, width, total):
    off = pl.multiple_of(index * width, width)
    before = pl.multiple_of(jnp.maximum(off - 128, 0), 128)
    after = pl.multiple_of(jnp.minimum(off + width, total - 128), 128)
    return off, before, after


def framed(left, mid, right, index, count):
    left = jnp.where(index > 0, left, 0.0)
    right = jnp.where(index < count - 1, right, 0.0)
    return jnp.concatenate([left, mid, right], axis=1)


CHUNK = 512


def ends_kernel(x_hbm, field_hbm, one_ref, two_ref, x_ref, field_ref, arrived):
    members, rows, width = x_ref.shape
    odd = is_odd()
    parts = arrived.shape[0] - 1
    size = width // parts

    def fetch(k):
        where = slice(k * size, (k + 1) * size)
        return pltpu.make_async_copy(x_hbm.at[:, :, where], x_ref.at[:, :, where], arrived.at[k])

    whole = pltpu.make_async_copy(field_hbm, field_ref, arrived.at[parts])
    whole.start()
    for k in range(parts):
        fetch(k).start()

    def put(where, low, high):
        one_ref[:, where] = jnp.where(odd, low, high).astype(BF16)
        two_ref[:, where] = jnp.where(odd, high, low).astype(BF16)

    piece = width // members

    def folded(row):
        lines = [field_ref[row : row + 1, s * piece : (s + 1) * piece] for s in range(members)]
        block = jnp.concatenate(lines, axis=0)
        return [part.astype(F32) for part in halves(block)]

    whole.wait()
    for k, (low, high) in enumerate(zip(folded(0), folded(rows - 1))):
        begin = 2 * width + k * piece
        put(slice(begin, begin + piece), low, high)

    def some(c, carry):
        off = pl.multiple_of(c * CHUNK, CHUNK)
        tall = [x_ref[m, :, pl.ds(off, CHUNK)].astype(F32) for m in range(members)]
        for k in range(2):
            low = jnp.concatenate([t[k : k + 1] for t in tall], axis=0)
            high = jnp.concatenate([t[rows - 2 + k : rows - 1 + k] for t in tall], axis=0)
            put(pl.ds(pl.multiple_of(k * width + off, CHUNK), CHUNK), low, high)
        return carry

    each = size // CHUNK
    for k in range(parts):
        fetch(k).wait()
        lax.fori_loop(k * each, (k + 1) * each, some, 0, unroll=2)


def ends(x, field):
    members, _, width = x.shape
    shape = jax.ShapeDtypeStruct((members, 2 * width + 2 * width // members), BF16)
    return pl.pallas_call(
        ends_kernel,
        out_shape=(
            shape,
            shape,
            jax.ShapeDtypeStruct(x.shape, x.dtype),
            jax.ShapeDtypeStruct(field.shape, field.dtype),
        ),
        in_specs=[pl.BlockSpec(memory_space=pltpu.HBM)] * 2,
        out_specs=tuple(vmem_specs(4)),
        scratch_shapes=[pltpu.SemaphoreType.DMA((5,))],
        compiler_params=params(),
        name="ends",
    )(*(pltpu.with_memory_space_constraint(v, pltpu.HBM) for v in (x, field)))


def first_pass(source, coef_ref, keep, index, width, spans, shift):
    off, before, after = edges_of(index, CHUNK, width)

    def load(r):
        pieces = [source(r, o, s) for o, s in ((before, 128), (off, CHUNK), (after, 128))]
        return framed(*pieces, index, width // CHUNK)

    for begin, count in spans:

        def put(r, value):
            keep(r, pl.ds(off, CHUNK), value)

        sweep(load, coef_ref, put, begin, count, shift, off, CHUNK)


def second_pass(coef_ref, pick, out_ref, index, width, spans, shift):
    cols = width // out_ref.shape[0]
    each = CHUNK // cols
    off, before, after = edges_of(index, CHUNK, width)

    def load(r):
        pieces = [pick(r, o, s) for o, s in ((before, 128), (off, CHUNK), (after, 128))]
        return framed(*pieces, index, width // CHUNK)

    def put(r, value):
        for k in range(each):
            out_ref[index * each + k, :, r * cols : (r + 1) * cols] = value[
                :, k * cols : (k + 1) * cols
            ].astype(BF16)

    for begin, count in spans:
        sweep(load, coef_ref, put, begin, count, shift, off, CHUNK)


def inner_kernel(x_ref, field_ref, out_ref, kept_ref, v1_ref):
    rows, _, width = x_ref.shape
    chunks = width // CHUNK
    kept = (1, 2, rows - 3, rows - 2)

    def first(c, carry):
        def source(r, off, size):
            return x_ref[r, :, pl.ds(off, size)].astype(F32)

        def keep(r, where, value):
            v1_ref[r + 1, :, where] = value
            if r in kept:
                kept_ref[kept.index(r), :, where] = value

        first_pass(source, field_ref, keep, c, width, ((1, rows - 2),), 0)
        return carry

    def pick(r, off, size):
        return v1_ref[r + 1, :, pl.ds(off, size)]

    def second(c, carry):
        second_pass(field_ref, pick, out_ref, c, width, ((2, rows - 4),), 0)
        return carry

    lax.fori_loop(0, chunks, first, 0, unroll=4)
    lax.fori_loop(0, chunks, second, 0, unroll=4)


def inner_forecast(x, field, patches):
    rows, members, width = x.shape
    return pl.pallas_call(
        inner_kernel,
        out_shape=(
            jax.ShapeDtypeStruct((patches, members, rows * width // patches), BF16),
            jax.ShapeDtypeStruct((4, members, width), F32),
        ),
        in_specs=vmem_specs(2),
        out_specs=tuple(vmem_specs(2)),
        scratch_shapes=[pltpu.VMEM((rows + 2, members, width), F32)],
        compiler_params=params(),
        name="inner",
    )(x, field)


def outer_kernel(x_ref, one_ref, two_ref, field_ref, part_ref, kept_ref, out_ref, v1_ref, coef_ref):
    rows, members, width = x_ref.shape
    del part_ref
    odd = is_odd()
    piece = width // members
    coef_ref[pl.ds(8, rows), :] = field_ref[...]
    one = one_ref[:, 2 * width :].astype(F32)
    two = two_ref[:, 2 * width :].astype(F32)
    one = one[:, :piece] + one[:, piece:]
    two = two[:, :piece] + two[:, piece:]
    low = jnp.where(odd, one, two)
    high = jnp.where(odd, two, one)
    for s in range(members):
        coef_ref[7:8, s * piece : (s + 1) * piece] = low[s : s + 1]
        coef_ref[8 + rows : 9 + rows, s * piece : (s + 1) * piece] = high[s : s + 1]

    def first(c, carry):
        def source(r, off, size):
            if 0 <= r < rows:
                return x_ref[r, :, pl.ds(off, size)].astype(F32)
            at = (r + 2 if r < 0 else r - rows) * width
            a = one_ref[:, pl.ds(at + off, size)].astype(F32)
            b = two_ref[:, pl.ds(at + off, size)].astype(F32)
            return jnp.where(odd, a, b) if r < 0 else jnp.where(odd, b, a)

        def keep(r, where, value):
            v1_ref[r + 1, :, where] = value

        first_pass(source, coef_ref, keep, c, width, ((-1, 2), (rows - 1, 2)), 8)
        return carry

    kept = (1, 2, rows - 3, rows - 2)

    def pick(r, off, size):
        if r in kept:
            return kept_ref[kept.index(r), :, pl.ds(off, size)]
        return v1_ref[r + 1, :, pl.ds(off, size)]

    def second(c, carry):
        second_pass(coef_ref, pick, out_ref, c, width, ((0, 2), (rows - 2, 2)), 8)
        return carry

    lax.fori_loop(0, width // CHUNK, first, 0, unroll=4)
    lax.fori_loop(0, width // CHUNK, second, 0, unroll=4)


def outer_forecast(x, one, two, field, part, kept):
    rows, members, width = x.shape
    return pl.pallas_call(
        outer_kernel,
        out_shape=jax.ShapeDtypeStruct(part.shape, BF16),
        in_specs=vmem_specs(6),
        out_specs=pl.BlockSpec(memory_space=pltpu.VMEM),
        scratch_shapes=[pltpu.VMEM((rows + 2, members, width), F32), pltpu.VMEM((rows + 16, width), F32)],
        input_output_aliases={4: 0},
        compiler_params=params(),
        name="outer",
    )(x, one, two, field, part, kept)


def gram_kernel(block_ref, site_ref, value_ref, weight_ref, out_ref):
    groups, each, cells = block_ref.shape
    members = groups * each
    count = site_ref.shape[1]
    half = members // 2
    step = 512
    site = site_ref[...]
    observed = jnp.zeros((members, count), F32)
    for c in range(cells // step):
        cell = lax.broadcasted_iota(jnp.int32, (step, count), 0) + c * step
        chosen = jnp.where(cell == site, 1.0, 0.0).astype(BF16)
        piece = block_ref[:, :, c * step : (c + 1) * step].reshape(members, step)
        observed += jnp.dot(piece, chosen, preferred_element_type=F32)
    mean = jnp.sum(observed, axis=0, keepdims=True) * (1.0 / members)
    root = jnp.sqrt(weight_ref[...])
    spread = ((observed - mean) * root).astype(BF16)
    innovation = ((value_ref[...] - mean) * root).astype(BF16)
    tail = jnp.broadcast_to(innovation.astype(F32), (16, count)).astype(BF16)
    left = jnp.concatenate([spread, tail], axis=0)
    both = lax.dot_general(left, spread, (((1,), (1,)), ((), ())), preferred_element_type=F32)
    low = both[half:members, half:]
    across = lax.broadcasted_iota(jnp.int32, (half, half), 0)
    along = lax.broadcasted_iota(jnp.int32, (half, half), 1)
    corner = jnp.sum(jnp.where(across == along, low, 0.0), axis=0, keepdims=True)
    out_ref[:half, :half] = jnp.where(across <= along, both[:half, :half], low)
    out_ref[:half, half:] = both[:half, half:]
    out_ref[half:, :] = both[members : members + 8]
    out_ref[half + 1 : half + 2, :half] = corner


def gram_of(blocks, sites, values, weights):
    members = blocks.shape[0] * blocks.shape[1]
    return pl.pallas_call(
        gram_kernel,
        out_shape=jax.ShapeDtypeStruct((members // 2 + 8, members), F32),
        in_specs=vmem_specs(4),
        out_specs=pl.BlockSpec(memory_space=pltpu.VMEM),
        compiler_params=params(),
        name="gram",
    )(blocks, sites, values, weights)


def unpacked(packed, half):
    across = lax.broadcasted_iota(jnp.int32, (half, half), 0)
    along = lax.broadcasted_iota(jnp.int32, (half, half), 1)
    block = packed[:half, :half]
    turned = block.T
    upper = jnp.where(across <= along, block, turned)
    lower = jnp.where(across > along, block, turned)
    lower = jnp.where(across == along, packed[half + 1 : half + 2, :half], lower)
    side = packed[:half, half:]
    return jnp.concatenate(
        [jnp.concatenate([upper, side], axis=1), jnp.concatenate([side.T, lower], axis=1)], axis=0
    )


def halves(value):
    high = value.astype(BF16)
    return high, (value - high.astype(F32)).astype(BF16)


def product(left, right):
    lh, ll = left
    rh, rl = right
    return (
        jnp.dot(lh, rh, preferred_element_type=F32)
        + jnp.dot(lh, rl, preferred_element_type=F32)
        + jnp.dot(ll, rh, preferred_element_type=F32)
    )


def root_kernel(one_ref, mid_ref, two_ref, out_ref, root_ref, inverse_ref):
    members = out_ref.shape[0]
    half = members // 2
    packed = mid_ref[...] + 0.5 * (one_ref[...] + two_ref[...])
    vector = packed[half : half + 8]
    gram = unpacked(packed, half)
    across = lax.broadcasted_iota(jnp.int32, (members, members), 0)
    along = lax.broadcasted_iota(jnp.int32, (members, members), 1)
    on_diagonal = across == along
    system = jnp.where(on_diagonal, gram + (members - 1.0), gram)
    squares = jnp.sum(jnp.sum(system * system, axis=0, keepdims=True), axis=1, keepdims=True)
    frob = jnp.sqrt(squares)
    root = system / frob

    def factor_of(value):
        return jnp.where(on_diagonal, 1.5 - 0.5 * value, -0.5 * value)

    def keep(ref, pair):
        ref[0], ref[1] = pair

    def kept(ref):
        return ref[0], ref[1]

    factor_h = halves(factor_of(root))
    keep(inverse_ref, factor_h)
    keep(root_ref, halves(product(halves(root), factor_h)))

    def newton(step, carry):
        factor_h = halves(factor_of(product(kept(inverse_ref), kept(root_ref))))
        new_root = product(kept(root_ref), factor_h)
        new_inverse = product(factor_h, kept(inverse_ref))
        keep(root_ref, halves(new_root))
        keep(inverse_ref, halves(new_inverse))
        return carry

    lax.fori_loop(1, ITERS - 1, newton, 0)
    factor_h = halves(factor_of(product(kept(inverse_ref), kept(root_ref))))
    inverse = product(factor_h, kept(inverse_ref))
    inverse_h = halves(inverse)
    weights = product(halves(product(halves(vector), inverse_h)), inverse_h) / frob
    scale = jnp.sqrt(members - 1.0) * lax.rsqrt(frob)
    out_ref[...] = (scale * inverse + weights[0:1]).astype(BF16)


def root_of(one, mid, two):
    members = mid.shape[1]
    return pl.pallas_call(
        root_kernel,
        out_shape=jax.ShapeDtypeStruct((members, members), BF16),
        in_specs=vmem_specs(3),
        out_specs=pl.BlockSpec(memory_space=pltpu.VMEM),
        scratch_shapes=[pltpu.VMEM((2, members, members), BF16)] * 2,
        compiler_params=params(),
        name="root",
    )(one, mid, two)


def center_kernel(block_ref, mean_ref, out_ref):
    groups, each, cells = block_ref.shape
    members = groups * each
    step = 256

    def one(c, carry):
        where = pl.ds(pl.multiple_of(c * step, step), step)
        cellwise = block_ref[:, :, where].astype(F32)
        mean = jnp.sum(jnp.sum(cellwise, axis=0), axis=0, keepdims=True) * (1.0 / members)
        mean_ref[:, where] = mean
        out_ref[:, where] = (cellwise.reshape(members, step) - mean).astype(BF16)
        return carry

    lax.fori_loop(0, cells // step, one, 0, unroll=2)


def centered(blocks):
    groups, each, cells = blocks.shape
    return pl.pallas_call(
        center_kernel,
        out_shape=(
            jax.ShapeDtypeStruct((1, cells), F32),
            jax.ShapeDtypeStruct((groups * each, cells), BF16),
        ),
        in_specs=vmem_specs(1),
        out_specs=tuple(vmem_specs(2)),
        compiler_params=params(),
        name="center",
    )(blocks)


def update_kernel(turned_ref, mean_ref, deviation_ref, out_ref):
    groups, each, cells = out_ref.shape
    step = 512

    def one(c, carry):
        where = pl.ds(pl.multiple_of(c * step, step), step)
        moved = jnp.dot(turned_ref[...], deviation_ref[:, where], preferred_element_type=F32)
        out_ref[:, :, where] = (mean_ref[:, where] + moved).reshape(groups, each, step).astype(BF16)
        return carry

    lax.fori_loop(0, cells // step, one, 0, unroll=2)


def update(turned, mean, deviation, shape):
    return pl.pallas_call(
        update_kernel,
        out_shape=jax.ShapeDtypeStruct(shape, BF16),
        in_specs=vmem_specs(3),
        out_specs=pl.BlockSpec(memory_space=pltpu.VMEM),
        compiler_params=params(),
        name="update",
    )(turned, mean, deviation)


def edges_kernel(block_ref, one_ref, two_ref):
    cols = one_ref.shape[2]
    odd = is_odd()
    for q in range(block_ref.shape[0]):
        first = block_ref[q, :, :cols].astype(F32)
        last = block_ref[q, :, -cols:].astype(F32)
        one_ref[q] = jnp.where(odd, first, last).astype(BF16)
        two_ref[q] = jnp.where(odd, last, first).astype(BF16)


def edges(blocks, cols):
    shape = jax.ShapeDtypeStruct((*blocks.shape[:2], cols), BF16)
    return pl.pallas_call(
        edges_kernel,
        out_shape=(shape, shape),
        in_specs=vmem_specs(1),
        out_specs=tuple(vmem_specs(2)),
        compiler_params=params(),
        name="edges",
    )(blocks)


def final_rows(source, coef_ref, put, index, cols, patches, spans):
    each = CHUNK // cols
    base = index * each
    off = pl.multiple_of(index * CHUNK, CHUNK)
    before = jnp.maximum(base - 1, 0)
    after = jnp.minimum(base + each, patches - 1)

    def load(r):
        left = source(r, before, cols - 128, cols)
        mid = jnp.concatenate([source(r, base + k, 0, cols) for k in range(each)], axis=1)
        return framed(left, mid, source(r, after, 0, 128), index, patches // each)

    for begin, count in spans:
        sweep(load, coef_ref, put, begin, count, 0, off, CHUNK)


def middle_kernel(block_ref, coef_ref, out_ref, ends_ref, lines_ref):
    patches, members, cells = block_ref.shape
    rows = coef_ref.shape[0]
    cols = cells // rows
    pitch = rows + 8
    lines_ref[...] = jnp.zeros_like(lines_ref)

    def one(c, carry):
        off = pl.multiple_of(c * CHUNK, CHUNK)

        def source(r, q, begin, end):
            if not 0 <= r < rows:
                return jnp.zeros((members, end - begin), F32)
            return block_ref[q, :, r * cols + begin : r * cols + end].astype(F32)

        def put(r, value):
            if r in (0, rows - 1):
                ends_ref[min(r, 1), :, pl.ds(off, CHUNK)] = value
                return
            for k in range(CHUNK // 128):
                lines_ref[k, pl.ds(r, members, stride=pitch), :] = value[:, k * 128 : (k + 1) * 128]

        final_rows(source, coef_ref, put, c, cols, patches, ((0, rows),))
        for m in range(members):
            tiles = [lines_ref[k, m * pitch : m * pitch + rows, :] for k in range(CHUNK // 128)]
            out_ref[m, :, pl.ds(off, CHUNK)] = jnp.concatenate(tiles, axis=1).astype(BF16)
        return carry

    lax.fori_loop(0, patches * cols // CHUNK, one, 0, unroll=2)


def middle_rows(blocks, coef):
    _, members, _ = blocks.shape
    rows, width = coef.shape
    return pl.pallas_call(
        middle_kernel,
        out_shape=(
            jax.ShapeDtypeStruct((members, rows, width), BF16),
            jax.ShapeDtypeStruct((2, members, width), F32),
        ),
        in_specs=vmem_specs(2),
        out_specs=tuple(vmem_specs(2)),
        scratch_shapes=[pltpu.VMEM((CHUNK // 128, members * (rows + 8), 128), F32)],
        compiler_params=params(),
        name="middle",
    )(blocks, coef)


def rim_kernel(one_ref, two_ref, coef_ref, part_ref, start_ref, out_ref, whole_ref, ends_ref, done):
    members, rows, width = part_ref.shape
    cols = one_ref.shape[2]
    each = CHUNK // cols
    chunks = width // CHUNK
    odd = is_odd()
    line = lax.broadcasted_iota(jnp.int32, (rows, CHUNK), 0)

    def move(c):
        where = pl.ds(pl.multiple_of(c * CHUNK, CHUNK), CHUNK)
        return pltpu.make_async_copy(whole_ref.at[:, :, where], out_ref.at[:, :, where], done.at[c])

    def one(c, carry):
        where = pl.ds(pl.multiple_of(c * CHUNK, CHUNK), CHUNK)
        a = jnp.concatenate([one_ref[c * each + k].astype(F32) for k in range(each)], axis=1)
        b = jnp.concatenate([two_ref[c * each + k].astype(F32) for k in range(each)], axis=1)
        for k, beside in enumerate((jnp.where(odd, a, b), jnp.where(odd, b, a))):
            r = k * (rows - 1)
            ends_ref[k, :, where] = start_ref[k, :, where] + coef_ref[r : r + 1, where] * beside
        for m in range(members):
            old = part_ref[m, :, where].astype(F32)
            new = jnp.where(line == 0, ends_ref[0, m : m + 1, where], old)
            new = jnp.where(line == rows - 1, ends_ref[1, m : m + 1, where], new)
            whole_ref[m, :, where] = new.astype(BF16)
        move(c).start()
        return carry

    lax.fori_loop(0, chunks, one, 0, unroll=4)

    def settle(c, carry):
        move(c).wait()
        return carry

    lax.fori_loop(0, chunks, settle, 0)


def rim_rows(one, two, coef, part, start):
    members, _, width = part.shape
    return pl.pallas_call(
        rim_kernel,
        out_shape=jax.ShapeDtypeStruct(part.shape, BF16),
        in_specs=vmem_specs(5),
        out_specs=pl.BlockSpec(memory_space=pl.ANY),
        scratch_shapes=[
            pltpu.VMEM(part.shape, BF16),
            pltpu.VMEM((2, members, width), F32),
            pltpu.SemaphoreType.DMA((width // CHUNK,)),
        ],
        compiler_params=params(),
        name="rim",
    )(one, two, coef, part, start)


def swaps(axis, in_one, in_two):
    count = lax.axis_size(axis)

    def pairs(first):
        both = [(i, i + 1) for i in range(first, count - 1, 2)]
        return both + [(j, i) for i, j in both]

    two = lax.ppermute(in_two, axis, pairs(1))
    one = lax.ppermute(in_one, axis, pairs(0))
    return one, two


def body(
    prior_samples,
    diffusivity_field,
    measured_site_position,
    measured_quantities,
    measurement_weightings,
):
    patches = lax.axis_size(MEM)
    cols = prior_samples.shape[2] // patches
    one, two, prior, field = ends(prior_samples, diffusivity_field)
    one, two = swaps("space", one, two)
    turned_prior = jnp.swapaxes(prior, 0, 1)
    part, kept = inner_forecast(turned_prior, field, patches)
    blocks = outer_forecast(turned_prior, one, two, field, part, kept)
    gathered = lax.all_to_all(blocks, MEM, 0, 0, tiled=True)
    own = gram_of(
        gathered, measured_site_position[0], measured_quantities[0], measurement_weightings[0]
    )
    one, two = swaps(MEM, own, own)
    mean, deviation = centered(gathered)
    band = own + 0.5 * (one + two)
    one, two = swaps("space", band, band)
    updated = update(root_of(one, band, two), mean, deviation, gathered.shape)
    returned = lax.all_to_all(updated, MEM, 0, 0, tiled=True)
    one, two = swaps("space", *edges(returned, cols))
    part, start = middle_rows(returned, field)
    return rim_rows(one, two, field, part, start)


def solution(mesh):
    finer = Mesh(
        mesh.devices.reshape(2, 8, 2, mesh.shape["space"]), ("mem_0", "mem_1", "mem_2", "space")
    )
    in_specs = (
        P(MEM, "space", None),
        P("space", None),
        P("space", MEM, None),
        P("space", MEM, None),
        P("space", MEM, None),
    )
    out_specs = P(MEM, "space", None)
    return jax.shard_map(body, mesh=finer, in_specs=in_specs, out_specs=out_specs, check_vma=False)
```

```python
import jax
import jax.numpy as jnp
from jax import lax
from jax.experimental import pallas as pl
from jax.experimental.pallas import tpu as pltpu
from jax.sharding import Mesh
from jax.sharding import PartitionSpec as P

ITERS = 10
MEM = ("mem_0", "mem_1", "mem_2")
F32 = jnp.float32
BF16 = jnp.bfloat16
VMEM_LIMIT = 24 << 20


def params():
    return pltpu.CompilerParams(vmem_limit_bytes=VMEM_LIMIT)


def is_odd():
    return lax.bitwise_and(lax.axis_index("space"), 1) > 0


def vmem_specs(count):
    return [pl.BlockSpec(memory_space=pltpu.VMEM) for _ in range(count)]


def sides(window):
    width = window.shape[1]
    both = pltpu.roll(window, 1, axis=1) + pltpu.roll(window, width - 1, axis=1)
    return both[:, 128 : width - 128]


def sweep(load, coef_ref, put, first, count, shift, off, width):
    above = load(first - 1)[:, 128 : 128 + width]
    here = load(first)
    for r in range(first, first + count):
        below = load(r + 1)
        mid = here[:, 128 : 128 + width]
        lap = (above + below[:, 128 : 128 + width]) + sides(here) - 4.0 * mid
        put(r, mid + coef_ref[r + shift : r + shift + 1, pl.ds(off, width)] * lap)
        above, here = mid, below


def edges_of(index, width, total):
    off = pl.multiple_of(index * width, width)
    before = pl.multiple_of(jnp.maximum(off - 128, 0), 128)
    after = pl.multiple_of(jnp.minimum(off + width, total - 128), 128)
    return off, before, after


def framed(left, mid, right, index, count):
    left = jnp.where(index > 0, left, 0.0)
    right = jnp.where(index < count - 1, right, 0.0)
    return jnp.concatenate([left, mid, right], axis=1)


CHUNK = 512


def ends_kernel(x_hbm, field_hbm, one_ref, two_ref, x_ref, field_ref, arrived):
    members, rows, width = x_ref.shape
    odd = is_odd()
    parts = arrived.shape[0] - 1
    size = width // parts

    def fetch(k):
        where = slice(k * size, (k + 1) * size)
        return pltpu.make_async_copy(x_hbm.at[:, :, where], x_ref.at[:, :, where], arrived.at[k])

    whole = pltpu.make_async_copy(field_hbm, field_ref, arrived.at[parts])
    whole.start()
    for k in range(parts):
        fetch(k).start()

    def put(where, low, high):
        one_ref[:, where] = jnp.where(odd, low, high).astype(BF16)
        two_ref[:, where] = jnp.where(odd, high, low).astype(BF16)

    piece = width // members

    def folded(row):
        lines = [field_ref[row : row + 1, s * piece : (s + 1) * piece] for s in range(members)]
        block = jnp.concatenate(lines, axis=0)
        return [part.astype(F32) for part in halves(block)]

    whole.wait()
    for k, (low, high) in enumerate(zip(folded(0), folded(rows - 1))):
        begin = 2 * width + k * piece
        put(slice(begin, begin + piece), low, high)

    def some(c, carry):
        off = pl.multiple_of(c * CHUNK, CHUNK)
        tall = [x_ref[m, :, pl.ds(off, CHUNK)].astype(F32) for m in range(members)]
        for k in range(2):
            low = jnp.concatenate([t[k : k + 1] for t in tall], axis=0)
            high = jnp.concatenate([t[rows - 2 + k : rows - 1 + k] for t in tall], axis=0)
            put(pl.ds(pl.multiple_of(k * width + off, CHUNK), CHUNK), low, high)
        return carry

    each = size // CHUNK
    for k in range(parts):
        fetch(k).wait()
        lax.fori_loop(k * each, (k + 1) * each, some, 0, unroll=2)


def ends(x, field):
    members, _, width = x.shape
    shape = jax.ShapeDtypeStruct((members, 2 * width + 2 * width // members), BF16)
    return pl.pallas_call(
        ends_kernel,
        out_shape=(
            shape,
            shape,
            jax.ShapeDtypeStruct(x.shape, x.dtype),
            jax.ShapeDtypeStruct(field.shape, field.dtype),
        ),
        in_specs=[pl.BlockSpec(memory_space=pltpu.HBM)] * 2,
        out_specs=tuple(vmem_specs(4)),
        scratch_shapes=[pltpu.SemaphoreType.DMA((9,))],
        compiler_params=params(),
        name="ends",
    )(*(pltpu.with_memory_space_constraint(v, pltpu.HBM) for v in (x, field)))


def first_pass(source, coef_ref, keep, index, width, spans, shift):
    off, before, after = edges_of(index, CHUNK, width)

    def load(r):
        pieces = [source(r, o, s) for o, s in ((before, 128), (off, CHUNK), (after, 128))]
        return framed(*pieces, index, width // CHUNK)

    for begin, count in spans:

        def put(r, value):
            keep(r, pl.ds(off, CHUNK), value)

        sweep(load, coef_ref, put, begin, count, shift, off, CHUNK)


def second_pass(coef_ref, pick, out_ref, index, width, spans, shift):
    cols = width // out_ref.shape[0]
    each = CHUNK // cols
    off, before, after = edges_of(index, CHUNK, width)

    def load(r):
        pieces = [pick(r, o, s) for o, s in ((before, 128), (off, CHUNK), (after, 128))]
        return framed(*pieces, index, width // CHUNK)

    def put(r, value):
        for k in range(each):
            out_ref[index * each + k, :, r * cols : (r + 1) * cols] = value[
                :, k * cols : (k + 1) * cols
            ].astype(BF16)

    for begin, count in spans:
        sweep(load, coef_ref, put, begin, count, shift, off, CHUNK)


def inner_kernel(x_ref, field_ref, out_ref, kept_ref, v1_ref):
    rows, _, width = x_ref.shape
    chunks = width // CHUNK
    kept = (1, 2, rows - 3, rows - 2)

    def first(c, carry):
        def source(r, off, size):
            return x_ref[r, :, pl.ds(off, size)].astype(F32)

        def keep(r, where, value):
            v1_ref[r + 1, :, where] = value
            if r in kept:
                kept_ref[kept.index(r), :, where] = value

        first_pass(source, field_ref, keep, c, width, ((1, rows - 2),), 0)
        return carry

    def pick(r, off, size):
        return v1_ref[r + 1, :, pl.ds(off, size)]

    def second(c, carry):
        second_pass(field_ref, pick, out_ref, c, width, ((2, rows - 4),), 0)
        return carry

    lax.fori_loop(0, chunks, first, 0, unroll=4)
    lax.fori_loop(0, chunks, second, 0, unroll=4)


def inner_forecast(x, field, patches):
    rows, members, width = x.shape
    return pl.pallas_call(
        inner_kernel,
        out_shape=(
            jax.ShapeDtypeStruct((patches, members, rows * width // patches), BF16),
            jax.ShapeDtypeStruct((4, members, width), F32),
        ),
        in_specs=vmem_specs(2),
        out_specs=tuple(vmem_specs(2)),
        scratch_shapes=[pltpu.VMEM((rows + 2, members, width), F32)],
        compiler_params=params(),
        name="inner",
    )(x, field)


def outer_kernel(x_ref, one_ref, two_ref, field_ref, part_ref, kept_ref, out_ref, v1_ref, coef_ref):
    rows, members, width = x_ref.shape
    del part_ref
    odd = is_odd()
    piece = width // members
    coef_ref[pl.ds(8, rows), :] = field_ref[...]
    one = one_ref[:, 2 * width :].astype(F32)
    two = two_ref[:, 2 * width :].astype(F32)
    one = one[:, :piece] + one[:, piece:]
    two = two[:, :piece] + two[:, piece:]
    low = jnp.where(odd, one, two)
    high = jnp.where(odd, two, one)
    for s in range(members):
        coef_ref[7:8, s * piece : (s + 1) * piece] = low[s : s + 1]
        coef_ref[8 + rows : 9 + rows, s * piece : (s + 1) * piece] = high[s : s + 1]

    def first(c, carry):
        def source(r, off, size):
            if 0 <= r < rows:
                return x_ref[r, :, pl.ds(off, size)].astype(F32)
            at = (r + 2 if r < 0 else r - rows) * width
            a = one_ref[:, pl.ds(at + off, size)].astype(F32)
            b = two_ref[:, pl.ds(at + off, size)].astype(F32)
            return jnp.where(odd, a, b) if r < 0 else jnp.where(odd, b, a)

        def keep(r, where, value):
            v1_ref[r + 1, :, where] = value

        first_pass(source, coef_ref, keep, c, width, ((-1, 2), (rows - 1, 2)), 8)
        return carry

    kept = (1, 2, rows - 3, rows - 2)

    def pick(r, off, size):
        if r in kept:
            return kept_ref[kept.index(r), :, pl.ds(off, size)]
        return v1_ref[r + 1, :, pl.ds(off, size)]

    def second(c, carry):
        second_pass(coef_ref, pick, out_ref, c, width, ((0, 2), (rows - 2, 2)), 8)
        return carry

    lax.fori_loop(0, width // CHUNK, first, 0, unroll=4)
    lax.fori_loop(0, width // CHUNK, second, 0, unroll=4)


def outer_forecast(x, one, two, field, part, kept):
    rows, members, width = x.shape
    return pl.pallas_call(
        outer_kernel,
        out_shape=jax.ShapeDtypeStruct(part.shape, BF16),
        in_specs=vmem_specs(6),
        out_specs=pl.BlockSpec(memory_space=pltpu.VMEM),
        scratch_shapes=[pltpu.VMEM((rows + 2, members, width), F32), pltpu.VMEM((rows + 16, width), F32)],
        input_output_aliases={4: 0},
        compiler_params=params(),
        name="outer",
    )(x, one, two, field, part, kept)


def gram_kernel(block_ref, site_ref, value_ref, weight_ref, out_ref):
    groups, each, cells = block_ref.shape
    members = groups * each
    count = site_ref.shape[1]
    half = members // 2
    step = 512
    site = site_ref[...]
    observed = jnp.zeros((members, count), F32)
    for c in range(cells // step):
        cell = lax.broadcasted_iota(jnp.int32, (step, count), 0) + c * step
        chosen = jnp.where(cell == site, 1.0, 0.0).astype(BF16)
        piece = block_ref[:, :, c * step : (c + 1) * step].reshape(members, step)
        observed += jnp.dot(piece, chosen, preferred_element_type=F32)
    mean = jnp.sum(observed, axis=0, keepdims=True) * (1.0 / members)
    root = jnp.sqrt(weight_ref[...])
    spread = ((observed - mean) * root).astype(BF16)
    innovation = ((value_ref[...] - mean) * root).astype(BF16)
    tail = jnp.broadcast_to(innovation.astype(F32), (16, count)).astype(BF16)
    left = jnp.concatenate([spread, tail], axis=0)
    both = lax.dot_general(left, spread, (((1,), (1,)), ((), ())), preferred_element_type=F32)
    low = both[half:members, half:]
    across = lax.broadcasted_iota(jnp.int32, (half, half), 0)
    along = lax.broadcasted_iota(jnp.int32, (half, half), 1)
    corner = jnp.sum(jnp.where(across == along, low, 0.0), axis=0, keepdims=True)
    out_ref[:half, :half] = jnp.where(across <= along, both[:half, :half], low)
    out_ref[:half, half:] = both[:half, half:]
    out_ref[half:, :] = both[members : members + 8]
    out_ref[half + 1 : half + 2, :half] = corner


def gram_of(blocks, sites, values, weights):
    members = blocks.shape[0] * blocks.shape[1]
    return pl.pallas_call(
        gram_kernel,
        out_shape=jax.ShapeDtypeStruct((members // 2 + 8, members), F32),
        in_specs=vmem_specs(4),
        out_specs=pl.BlockSpec(memory_space=pltpu.VMEM),
        compiler_params=params(),
        name="gram",
    )(blocks, sites, values, weights)


def unpacked(packed, half):
    across = lax.broadcasted_iota(jnp.int32, (half, half), 0)
    along = lax.broadcasted_iota(jnp.int32, (half, half), 1)
    block = packed[:half, :half]
    turned = block.T
    upper = jnp.where(across <= along, block, turned)
    lower = jnp.where(across > along, block, turned)
    lower = jnp.where(across == along, packed[half + 1 : half + 2, :half], lower)
    side = packed[:half, half:]
    return jnp.concatenate(
        [jnp.concatenate([upper, side], axis=1), jnp.concatenate([side.T, lower], axis=1)], axis=0
    )


def halves(value):
    high = value.astype(BF16)
    return high, (value - high.astype(F32)).astype(BF16)


def product(left, right):
    lh, ll = left
    rh, rl = right
    return jnp.dot(
        jnp.concatenate([lh, lh, ll], axis=1),
        jnp.concatenate([rh, rl, rh], axis=0),
        preferred_element_type=F32,
    )


def root_kernel(one_ref, mid_ref, two_ref, out_ref, root_ref, inverse_ref):
    members = out_ref.shape[0]
    half = members // 2
    packed = mid_ref[...] + 0.5 * (one_ref[...] + two_ref[...])
    vector = packed[half : half + 8]
    gram = unpacked(packed, half)
    across = lax.broadcasted_iota(jnp.int32, (members, members), 0)
    along = lax.broadcasted_iota(jnp.int32, (members, members), 1)
    on_diagonal = across == along
    system = jnp.where(on_diagonal, gram + (members - 1.0), gram)
    squares = jnp.sum(jnp.sum(system * system, axis=0, keepdims=True), axis=1, keepdims=True)
    frob = jnp.sqrt(squares)
    root = system / frob

    def factor_of(value):
        return jnp.where(on_diagonal, 1.5 - 0.5 * value, -0.5 * value)

    def keep(ref, pair):
        ref[0], ref[1] = pair

    def kept(ref):
        return ref[0], ref[1]

    factor_h = halves(factor_of(root))
    keep(inverse_ref, factor_h)
    keep(root_ref, halves(product(halves(root), factor_h)))

    def newton(step, carry):
        factor_h = halves(factor_of(product(kept(inverse_ref), kept(root_ref))))
        new_root = product(kept(root_ref), factor_h)
        new_inverse = product(factor_h, kept(inverse_ref))
        keep(root_ref, halves(new_root))
        keep(inverse_ref, halves(new_inverse))
        return carry

    lax.fori_loop(1, ITERS - 1, newton, 0)
    factor_h = halves(factor_of(product(kept(inverse_ref), kept(root_ref))))
    inverse = product(factor_h, kept(inverse_ref))
    inverse_h = halves(inverse)
    weights = product(halves(product(halves(vector), inverse_h)), inverse_h) / frob
    scale = jnp.sqrt(members - 1.0) * lax.rsqrt(frob)
    out_ref[...] = (scale * inverse + weights[0:1]).astype(BF16)


def root_of(one, mid, two):
    members = mid.shape[1]
    return pl.pallas_call(
        root_kernel,
        out_shape=jax.ShapeDtypeStruct((members, members), BF16),
        in_specs=vmem_specs(3),
        out_specs=pl.BlockSpec(memory_space=pltpu.VMEM),
        scratch_shapes=[pltpu.VMEM((2, members, members), BF16)] * 2,
        compiler_params=params(),
        name="root",
    )(one, mid, two)


def center_kernel(block_ref, mean_ref, out_ref):
    groups, each, cells = block_ref.shape
    members = groups * each
    step = 256

    def one(c, carry):
        where = pl.ds(pl.multiple_of(c * step, step), step)
        cellwise = block_ref[:, :, where].astype(F32)
        mean = jnp.sum(jnp.sum(cellwise, axis=0), axis=0, keepdims=True) * (1.0 / members)
        mean_ref[:, where] = mean
        out_ref[:, where] = (cellwise.reshape(members, step) - mean).astype(BF16)
        return carry

    lax.fori_loop(0, cells // step, one, 0, unroll=2)


def centered(blocks):
    groups, each, cells = blocks.shape
    return pl.pallas_call(
        center_kernel,
        out_shape=(
            jax.ShapeDtypeStruct((1, cells), F32),
            jax.ShapeDtypeStruct((groups * each, cells), BF16),
        ),
        in_specs=vmem_specs(1),
        out_specs=tuple(vmem_specs(2)),
        compiler_params=params(),
        name="center",
    )(blocks)


def update_kernel(turned_ref, mean_ref, deviation_ref, out_ref):
    groups, each, cells = out_ref.shape
    step = 512

    def one(c, carry):
        where = pl.ds(pl.multiple_of(c * step, step), step)
        moved = jnp.dot(turned_ref[...], deviation_ref[:, where], preferred_element_type=F32)
        out_ref[:, :, where] = (mean_ref[:, where] + moved).reshape(groups, each, step).astype(BF16)
        return carry

    lax.fori_loop(0, cells // step, one, 0, unroll=2)


def update(turned, mean, deviation, shape):
    return pl.pallas_call(
        update_kernel,
        out_shape=jax.ShapeDtypeStruct(shape, BF16),
        in_specs=vmem_specs(3),
        out_specs=pl.BlockSpec(memory_space=pltpu.VMEM),
        compiler_params=params(),
        name="update",
    )(turned, mean, deviation)


def edges_kernel(block_ref, one_ref, two_ref):
    cols = one_ref.shape[2]
    odd = is_odd()
    for q in range(block_ref.shape[0]):
        first = block_ref[q, :, :cols].astype(F32)
        last = block_ref[q, :, -cols:].astype(F32)
        one_ref[q] = jnp.where(odd, first, last).astype(BF16)
        two_ref[q] = jnp.where(odd, last, first).astype(BF16)


def edges(blocks, cols):
    shape = jax.ShapeDtypeStruct((*blocks.shape[:2], cols), BF16)
    return pl.pallas_call(
        edges_kernel,
        out_shape=(shape, shape),
        in_specs=vmem_specs(1),
        out_specs=tuple(vmem_specs(2)),
        compiler_params=params(),
        name="edges",
    )(blocks)


def final_rows(source, coef_ref, put, index, cols, patches, spans):
    each = CHUNK // cols
    base = index * each
    off = pl.multiple_of(index * CHUNK, CHUNK)
    before = jnp.maximum(base - 1, 0)
    after = jnp.minimum(base + each, patches - 1)

    def load(r):
        left = source(r, before, cols - 128, cols)
        mid = jnp.concatenate([source(r, base + k, 0, cols) for k in range(each)], axis=1)
        return framed(left, mid, source(r, after, 0, 128), index, patches // each)

    for begin, count in spans:
        sweep(load, coef_ref, put, begin, count, 0, off, CHUNK)


def middle_kernel(block_ref, coef_ref, out_ref, ends_ref, lines_ref):
    patches, members, cells = block_ref.shape
    rows = coef_ref.shape[0]
    cols = cells // rows
    pitch = rows + 8
    lines_ref[...] = jnp.zeros_like(lines_ref)

    def one(c, carry):
        off = pl.multiple_of(c * CHUNK, CHUNK)

        def source(r, q, begin, end):
            if not 0 <= r < rows:
                return jnp.zeros((members, end - begin), F32)
            return block_ref[q, :, r * cols + begin : r * cols + end].astype(F32)

        def put(r, value):
            if r in (0, rows - 1):
                ends_ref[min(r, 1), :, pl.ds(off, CHUNK)] = value
                return
            for k in range(CHUNK // 128):
                lines_ref[k, pl.ds(r, members, stride=pitch), :] = value[:, k * 128 : (k + 1) * 128]

        final_rows(source, coef_ref, put, c, cols, patches, ((0, rows),))
        for m in range(members):
            tiles = [lines_ref[k, m * pitch : m * pitch + rows, :] for k in range(CHUNK // 128)]
            out_ref[m, :, pl.ds(off, CHUNK)] = jnp.concatenate(tiles, axis=1).astype(BF16)
        return carry

    lax.fori_loop(0, patches * cols // CHUNK, one, 0, unroll=2)


def middle_rows(blocks, coef):
    _, members, _ = blocks.shape
    rows, width = coef.shape
    return pl.pallas_call(
        middle_kernel,
        out_shape=(
            jax.ShapeDtypeStruct((members, rows, width), BF16),
            jax.ShapeDtypeStruct((2, members, width), F32),
        ),
        in_specs=vmem_specs(2),
        out_specs=tuple(vmem_specs(2)),
        scratch_shapes=[pltpu.VMEM((CHUNK // 128, members * (rows + 8), 128), F32)],
        compiler_params=params(),
        name="middle",
    )(blocks, coef)


def rim_kernel(one_ref, two_ref, coef_ref, part_ref, start_ref, out_ref, whole_ref, ends_ref, done):
    members, rows, width = part_ref.shape
    cols = one_ref.shape[2]
    each = CHUNK // cols
    chunks = width // CHUNK
    odd = is_odd()
    line = lax.broadcasted_iota(jnp.int32, (rows, CHUNK), 0)

    def move(c):
        where = pl.ds(pl.multiple_of(c * CHUNK, CHUNK), CHUNK)
        return pltpu.make_async_copy(whole_ref.at[:, :, where], out_ref.at[:, :, where], done.at[c])

    def one(c, carry):
        where = pl.ds(pl.multiple_of(c * CHUNK, CHUNK), CHUNK)
        a = jnp.concatenate([one_ref[c * each + k].astype(F32) for k in range(each)], axis=1)
        b = jnp.concatenate([two_ref[c * each + k].astype(F32) for k in range(each)], axis=1)
        for k, beside in enumerate((jnp.where(odd, a, b), jnp.where(odd, b, a))):
            r = k * (rows - 1)
            ends_ref[k, :, where] = start_ref[k, :, where] + coef_ref[r : r + 1, where] * beside
        for m in range(members):
            old = part_ref[m, :, where].astype(F32)
            new = jnp.where(line == 0, ends_ref[0, m : m + 1, where], old)
            new = jnp.where(line == rows - 1, ends_ref[1, m : m + 1, where], new)
            whole_ref[m, :, where] = new.astype(BF16)
        move(c).start()
        return carry

    lax.fori_loop(0, chunks, one, 0, unroll=4)

    def settle(c, carry):
        move(c).wait()
        return carry

    lax.fori_loop(0, chunks, settle, 0)


def rim_rows(one, two, coef, part, start):
    members, _, width = part.shape
    return pl.pallas_call(
        rim_kernel,
        out_shape=jax.ShapeDtypeStruct(part.shape, BF16),
        in_specs=vmem_specs(5),
        out_specs=pl.BlockSpec(memory_space=pl.ANY),
        scratch_shapes=[
            pltpu.VMEM(part.shape, BF16),
            pltpu.VMEM((2, members, width), F32),
            pltpu.SemaphoreType.DMA((width // CHUNK,)),
        ],
        compiler_params=params(),
        name="rim",
    )(one, two, coef, part, start)


def swaps(axis, in_one, in_two):
    count = lax.axis_size(axis)

    def pairs(first):
        both = [(i, i + 1) for i in range(first, count - 1, 2)]
        return both + [(j, i) for i, j in both]

    two = lax.ppermute(in_two, axis, pairs(1))
    one = lax.ppermute(in_one, axis, pairs(0))
    return one, two


def body(
    prior_samples,
    diffusivity_field,
    measured_site_position,
    measured_quantities,
    measurement_weightings,
):
    patches = lax.axis_size(MEM)
    cols = prior_samples.shape[2] // patches
    one, two, prior, field = ends(prior_samples, diffusivity_field)
    one, two = swaps("space", one, two)
    turned_prior = jnp.swapaxes(prior, 0, 1)
    part, kept = inner_forecast(turned_prior, field, patches)
    blocks = outer_forecast(turned_prior, one, two, field, part, kept)
    gathered = lax.all_to_all(blocks, MEM, 0, 0, tiled=True)
    own = gram_of(
        gathered, measured_site_position[0], measured_quantities[0], measurement_weightings[0]
    )
    one, two = swaps(MEM, own, own)
    mean, deviation = centered(gathered)
    band = own + 0.5 * (one + two)
    one, two = swaps("space", band, band)
    updated = update(root_of(one, band, two), mean, deviation, gathered.shape)
    returned = lax.all_to_all(updated, MEM, 0, 0, tiled=True)
    one, two = swaps("space", *edges(returned, cols))
    part, start = middle_rows(returned, field)
    return rim_rows(one, two, field, part, start)


def solution(mesh):
    finer = Mesh(
        mesh.devices.reshape(2, 8, 2, mesh.shape["space"]), ("mem_0", "mem_1", "mem_2", "space")
    )
    in_specs = (
        P(MEM, "space", None),
        P("space", None),
        P("space", MEM, None),
        P("space", MEM, None),
        P("space", MEM, None),
    )
    out_specs = P(MEM, "space", None)
    return jax.shard_map(body, mesh=finer, in_specs=in_specs, out_specs=out_specs, check_vma=False)
```
